256 devices in a mesh: blk: 32 (over z, y), rep: 8 (over x, core).
Axes of the slice: x: 4, y: 4, z: 8, core: 2. Of those that a mesh axis runs over, the one named last changes fastest.
Arguments:
- tensor_blocks: bfloat16 [512, 128, 128, 128], P(('blk', 'rep')), may hold values from -15 to 15
- triples: int32 [512, 3], P(('blk', 'rep')), may hold values from 0 to 63, as said below
- slot_count: int32 [256], P(('blk', 'rep')), may hold values from 1 to 2, as said below
- factor: bfloat16 [8192, 256], P('blk', 'rep'), may hold values from -0.19743253 to 0.19743253
Outputs:
- gradient: float32 [8192, 256], P('blk', 'rep')
The draws below stay inside these ranges and needn't reach their ends.
Inputs may be any that keep to these rules, and one draw needn't show every extreme that they name: `triples`: each row is i >= j >= k; equal indices occur; the different row blocks named by the 2 slots of one device have different values of block // 2. `slot_count`: the first device's entry is 2.
All inputs are finite; a program needn't handle non-finite values.
Results may differ from the reference program's by a relative error of at most 0.003.
Values may be sent and summed in bfloat16 or wider, within the bound.
No kernel may reach another device: no remote copies, remote signals or barrier semaphores. Data moves between devices by JAX's collectives and lax.ppermute only.
A program may use at most 128 MiB of HBM per device.

```python
import jax
import jax.numpy as jnp
from jax import lax

BS = 128
R = 256
BLK_DEV = 2
SLOTS = 2
NB = 64
MODES = 8192
HOLDERS = 256


def draw_triples(key, part):
    keys = jax.random.split(jax.random.fold_in(key, 11), 5)
    owner_total = NB // BLK_DEV
    scores = jax.random.randint(keys[0], (HOLDERS, owner_total), 0, 1 << 20)
    scores = scores * owner_total + jnp.arange(owner_total, dtype=jnp.int32)[None, :]
    owners = jnp.argsort(scores, axis=1)[:, :3 * SLOTS].astype(jnp.int32)
    local = jax.random.randint(keys[1], (HOLDERS, 3 * SLOTS), 0, BLK_DEV)
    picks = (owners * BLK_DEV + local).reshape(HOLDERS * SLOTS, 3)
    first_raw = picks[:, 0]
    second_raw = picks[:, 1]
    third_raw = picks[:, 2]
    shape = (HOLDERS * SLOTS,)
    tie_upper = jax.random.randint(keys[3], shape, 0, 4) == 0
    tie_lower = jax.random.randint(keys[4], shape, 0, 4) == 0
    second_raw = jnp.where(tie_upper, first_raw, second_raw)
    third_raw = jnp.where(tie_lower, second_raw, third_raw)
    highest = jnp.maximum(jnp.maximum(first_raw, second_raw), third_raw)
    lowest = jnp.minimum(jnp.minimum(first_raw, second_raw), third_raw)
    middle = first_raw + second_raw + third_raw - highest - lowest
    return jnp.stack([highest, middle, lowest], axis=1).astype(jnp.int32)


def draw_slot_count(key, part):
    counts = jax.random.randint(jax.random.fold_in(key, 23), (HOLDERS,), 1, SLOTS + 1)
    return counts.at[0].set(SLOTS).astype(jnp.int32)


def draw_factor(key, part):
    keys = jax.random.split(jax.random.fold_in(key, 37), 3)
    scale = (8.0 * MODES * MODES) ** (-0.2)
    noise = jnp.clip(jax.random.normal(keys[0], (MODES, R), jnp.float32), -6.0, 6.0)
    shared = jnp.clip(jax.random.normal(keys[1], (MODES, 1), jnp.float32), -6.0, 6.0)
    column_scale = jax.random.uniform(keys[2], (1, R), jnp.float32, 0.5, 1.5)
    values = noise + 0.5 * shared * column_scale
    return (scale * values).astype(jnp.bfloat16)


def block_scale(rng, dims, pieces, least, top_value):
    gain, own = 1.0, jax.random.fold_in(rng, 6)
    for axis_at, shards_of in pieces:
        steps = jnp.exp(jax.random.uniform(jax.random.fold_in(own, axis_at), (shards_of,), jnp.float32, least / len(pieces), top_value / len(pieces)))
        gain = gain * jnp.repeat(steps, dims[axis_at] // shards_of).reshape([-1 if axis == axis_at else 1 for axis in range(len(dims))])
    return gain


def centred(rng, shape, scale, reach, cuts=(), held_as=jnp.bfloat16):
    factor_of = block_scale(rng, shape, cuts, -0.22, 0.18) if cuts else 1.0
    values = jax.random.normal(rng, shape, jnp.float32) * scale * factor_of
    return jnp.minimum(jnp.maximum(values, -reach), reach).astype(held_as)


def setup_inputs(seed: int = 0) -> dict:
    splits = jax.random.split(jax.random.key(seed), 5)
    tensor_blocks = centred(splits[0], (HOLDERS * SLOTS, BS, BS, BS), 3.0, 15.0, ((0, 256),))
    triples = draw_triples(jax.random.fold_in(splits[4], 71), 0)
    slot_count = draw_slot_count(jax.random.fold_in(splits[4], 71), 0)
    factor = draw_factor(jax.random.fold_in(splits[4], 71), 0)
    return {"tensor_blocks": tensor_blocks, "triples": triples, "slot_count": slot_count, "factor": factor}


def side_weights(triples):
    first_idx = triples[:, 0]
    second_idx = triples[:, 1]
    third_idx = triples[:, 2]
    same_upper = first_idx == second_idx
    same_lower = second_idx == third_idx
    apart = jnp.logical_and(jnp.logical_not(same_upper), jnp.logical_not(same_lower))
    every = jnp.logical_and(same_upper, same_lower)
    base = jnp.where(apart, 2.0, 1.0).astype(jnp.float32)
    dropped = jnp.where(every, 0.0, base).astype(jnp.float32)
    return jnp.stack([base, dropped, dropped], axis=1)


def contract(block, upper, middle, lower):
    edge_size = block.shape[0]
    rank_width = upper.shape[1]
    by_lower = jnp.dot(block.reshape(edge_size * edge_size, edge_size), lower,
                       preferred_element_type=jnp.float32,
                       precision=lax.Precision.HIGHEST).reshape(edge_size, edge_size, rank_width)
    by_upper = lax.dot_general(block.reshape(edge_size, edge_size * edge_size), upper,
                               (((0,), (0,)), ((), ())), preferred_element_type=jnp.float32,
                               precision=lax.Precision.HIGHEST).reshape(edge_size, edge_size, rank_width)
    upper_wide = upper.astype(jnp.float32)
    middle_wide = middle.astype(jnp.float32)
    to_first = jnp.einsum("abr,br->ar", by_lower, middle_wide, precision=lax.Precision.HIGHEST)
    to_second = jnp.einsum("abr,ar->br", by_lower, upper_wide, precision=lax.Precision.HIGHEST)
    to_third = jnp.einsum("bcr,br->cr", by_upper, middle_wide, precision=lax.Precision.HIGHEST)
    return to_first, to_second, to_third


def reference(tensor_blocks, triples, slot_count, factor):
    blocks = factor.astype(jnp.float32).reshape(NB, BS, R)
    slot_ids = jnp.arange(HOLDERS * SLOTS, dtype=jnp.int32)
    holder_of = (slot_ids // SLOTS).astype(jnp.int32)
    position = (slot_ids % SLOTS).astype(jnp.int32)
    alive = (position < slot_count[holder_of]).astype(jnp.float32)
    weights = side_weights(triples) * alive[:, None]

    def accumulate(total, block, triple, weight):
        upper = blocks[triple[0]]
        middle = blocks[triple[1]]
        lower = blocks[triple[2]]
        to_first, to_second, to_third = contract(block.astype(jnp.float32), upper, middle, lower)
        total = total.at[triple[0]].add(weight[0] * to_first)
        total = total.at[triple[1]].add(weight[1] * to_second)
        total = total.at[triple[2]].add(weight[2] * to_third)
        return total

    def step(total, item):
        block, triple, weight, flag = item
        total = lax.cond(flag > 0.5,
                         lambda accum: accumulate(accum, block, triple, weight),
                         lambda accum: accum, total)
        return total, None

    start = jnp.zeros((NB, BS, R), jnp.float32)
    moment, _ = lax.scan(step, start, (tensor_blocks, triples, weights, alive))
    gram = jnp.dot(factor.T, factor, preferred_element_type=jnp.float32)
    hadamard = gram * gram
    fitted = jnp.dot(factor.astype(jnp.float32), hadamard, preferred_element_type=jnp.float32,
                     precision=lax.Precision.HIGHEST)
    return fitted - moment.reshape(MODES, R)
```

```python
import jax
import jax.numpy as jnp
from jax import lax
from jax.experimental import pallas as pl
from jax.experimental.pallas import tpu as pltpu
from jax.sharding import Mesh
from jax.sharding import PartitionSpec as P

BLK = ("blk_0", "blk_1")
BLK_REP = ("blk_0", "blk_1", "rep")

BS = 128
CHUNK = 8
F32 = jnp.float32
BF16 = jnp.bfloat16
VMEM = pltpu.VMEM
SMEM = pltpu.SMEM


def whole(space=VMEM):
    return pl.BlockSpec(memory_space=space)


def select_kernel(names, table, own, out):
    reps, named = names.shape
    own_count = own.shape[0]
    gram_count = table.shape[0] // reps
    for peer in range(reps):
        for t in range(named):
            out[peer, t] = table[names[peer, t]]
        for t in range(own_count):
            out[peer, named + t] = own[t]
        for t in range(gram_count):
            out[peer, named + own_count + t] = table[peer * gram_count + t]


def contract_kernel(triples, count, x, sel, out, fac, lower_s, middle_s, y1, y2, y3):
    reps, tiles, width, _ = sel.shape
    rank = reps * width
    slot = pl.program_id(0)
    step = pl.program_id(1)
    steps = pl.num_programs(1)
    named = 3 * pl.num_programs(0)

    def column_major(t):
        return sel[:, t].reshape(rank, BS)

    @pl.when(step == 0)
    def _():
        for side in range(3):
            tile = sel[:, pl.ds(slot * 3 + side, 1)].reshape(rank, BS)
            fac[side] = tile.astype(F32).T
        y2[...] = jnp.zeros_like(y2)
        y3[...] = jnp.zeros_like(y3)

    @pl.when((slot == 0) & (step == 0))
    def _():
        gram = jnp.zeros((rank, rank), F32)
        for t in range(8, tiles):
            part = column_major(t)
            gram = gram + lax.dot_general(
                part, part, (((1,), (1,)), ((), ())), preferred_element_type=F32
            )
        for half in range(rank // BS):
            out[:, 6 + half] = gram[:, half * BS : (half + 1) * BS].reshape(reps, width, BS)

    blocks = x[0]
    lower = fac[2].astype(BF16)
    middle = fac[1].astype(BF16)
    lower_s[...] = jnp.dot(
        blocks.reshape(CHUNK * BS, BS), lower, preferred_element_type=F32
    ).reshape(CHUNK, BS, rank)
    turned = jnp.concatenate([blocks[a].T for a in range(CHUNK)], axis=0)
    middle_s[...] = jnp.dot(turned, middle, preferred_element_type=F32).reshape(CHUNK, BS, rank)

    row0 = pl.multiple_of(step * CHUNK, CHUNK)
    for half in range(rank // BS):
        cols = slice(half * BS, (half + 1) * BS)
        upper_rows = fac[0, pl.ds(row0, CHUNK), cols]
        spread = [jnp.broadcast_to(upper_rows[a : a + 1], (8, BS)) for a in range(CHUNK)]
        sums = [jnp.zeros((8, BS), F32) for _ in range(CHUNK)]
        for b in range(0, BS, 8):
            rows = slice(b, b + 8)
            other = fac[1, rows, cols]
            second = y2[rows, cols]
            third = y3[rows, cols]
            for a in range(CHUNK):
                value = lower_s[a, rows, cols]
                sums[a] = sums[a] + value * other
                second = second + value * spread[a]
                third = third + middle_s[a, rows, cols] * spread[a]
            y2[rows, cols] = second
            y3[rows, cols] = third
        y1[pl.ds(row0, CHUNK), cols] = jnp.concatenate(
            [jnp.sum(sums[a], axis=0, keepdims=True) for a in range(CHUNK)], axis=0
        )

    @pl.when(step == steps - 1)
    def _():
        i, j, k = triples[slot, 0], triples[slot, 1], triples[slot, 2]
        upper_tie = i == j
        lower_tie = j == k
        alive = jnp.where(slot < count[0], 1.0, 0.0)
        base = jnp.where(upper_tie | lower_tie, 1.0, 2.0) * alive
        dropped = jnp.where(upper_tie & lower_tie, 0.0, base)
        for side, (value, weight) in enumerate(((y1, base), (y2, dropped), (y3, dropped))):
            out[:, pl.ds(slot * 3 + side, 1)] = (value[...].T * weight).reshape(
                reps, 1, width, BS
            )


def scatter_kernel(names, parts, own, total, fitted):
    reps, named = names.shape
    width = parts.shape[2]
    rank = reps * width
    total[...] = jnp.zeros_like(total)
    for peer in range(reps):
        for t in range(named):
            at = names[peer, t]
            total[at] = total[at] + parts[peer, t]
    halves = []
    for half in range(rank // BS):
        gram = parts[0, named + half]
        for peer in range(1, reps):
            gram = gram + parts[peer, named + half]
        halves.append(gram)
    gram = jnp.concatenate(halves, axis=1)
    rest = gram * gram
    pieces = []
    for _ in range(3):
        piece = rest.astype(BF16)
        rest = rest - piece.astype(F32)
        pieces.append(piece)
    for t in range(fitted.shape[0]):
        rows = own[:, named + t].reshape(rank, BS)
        value = jnp.dot(pieces[2], rows, preferred_element_type=F32)
        value = value + jnp.dot(pieces[1], rows, preferred_element_type=F32)
        fitted[t] = value + jnp.dot(pieces[0], rows, preferred_element_type=F32)


def finish_kernel(arrived, fitted, out):
    for t in range(fitted.shape[0]):
        total = arrived[0, t]
        for source in range(1, arrived.shape[0]):
            total = total + arrived[source, t]
        out[t * BS : (t + 1) * BS, :] = (fitted[t] - total).T


def gathered(array, axis):
    peers = lax.axis_size(axis)
    return lax.all_to_all(
        jnp.broadcast_to(array[None], (peers, *array.shape)), axis, 0, 0, tiled=True
    )


def shards(tensor_blocks, triples, slot_count, factor):
    slots = tensor_blocks.shape[0]
    reps = lax.axis_size("rep")
    owners = lax.axis_size(BLK)
    rows, width = factor.shape
    per_owner = rows // BS
    rank = reps * width
    named = 3 * slots
    own = factor.T.reshape(width, per_owner, BS).swapaxes(0, 1)
    names = lax.all_gather(triples.reshape(1, named), "rep", axis=0, tiled=True)
    near = gathered(own, "blk_1")
    table = gathered(near, "blk_0").reshape(owners * per_owner, width, BS)
    gram_count = owners * per_owner // reps
    tiles = named + per_owner + gram_count
    chosen = pl.pallas_call(
        select_kernel,
        out_shape=jax.ShapeDtypeStruct((reps, tiles, width, BS), BF16),
        in_specs=[whole(SMEM), whole(), whole()],
        out_specs=whole(),
        name="select",
    )(names, table, own)
    chosen = lax.all_to_all(chosen, "rep", 0, 0, tiled=True)
    steps = BS // CHUNK
    parts = pl.pallas_call(
        contract_kernel,
        grid=(slots, steps),
        out_shape=jax.ShapeDtypeStruct((reps, named + rank // BS, width, BS), F32),
        in_specs=[
            whole(SMEM),
            whole(SMEM),
            pl.BlockSpec((1, CHUNK, BS, BS), lambda s, c: (s, c, 0, 0)),
            whole(),
        ],
        out_specs=whole(),
        scratch_shapes=[
            VMEM((3, BS, rank), F32),
            VMEM((CHUNK, BS, rank), F32),
            VMEM((CHUNK, BS, rank), F32),
            VMEM((BS, rank), F32),
            VMEM((BS, rank), F32),
            VMEM((BS, rank), F32),
        ],
        name="contract",
    )(triples, slot_count, tensor_blocks, chosen)
    parts = lax.all_to_all(parts, "rep", 0, 0, tiled=True)
    total, fitted = pl.pallas_call(
        scatter_kernel,
        out_shape=(
            jax.ShapeDtypeStruct((owners * per_owner, width, BS), F32),
            jax.ShapeDtypeStruct((per_owner, width, BS), F32),
        ),
        in_specs=[whole(SMEM), whole(), whole()],
        out_specs=(whole(), whole()),
        name="scatter",
    )(names, parts, chosen)
    arrived = lax.all_to_all(
        total.reshape(owners, per_owner, width, BS), BLK, 0, 0, tiled=True
    )
    return pl.pallas_call(
        finish_kernel,
        out_shape=jax.ShapeDtypeStruct((rows, width), F32),
        in_specs=[whole(), whole()],
        out_specs=whole(),
        name="finish",
    )(arrived, fitted)


def solution(mesh):
    split = Mesh(mesh.devices.reshape(8, 4, mesh.shape["rep"]), ("blk_0", "blk_1", "rep"))
    in_specs = (P(BLK_REP, None, None, None), P(BLK_REP, None), P(BLK_REP), P(BLK, "rep"))
    out_specs = P(BLK, "rep")
    return jax.shard_map(
        shards, mesh=split, in_specs=in_specs, out_specs=out_specs, check_vma=False
    )
```

```python
import jax
import jax.numpy as jnp
from jax import lax
from jax.experimental import pallas as pl
from jax.experimental.pallas import tpu as pltpu
from jax.sharding import Mesh
from jax.sharding import PartitionSpec as P

BLK = ("blk_0", "blk_1")
BLK_REP = ("blk_0", "blk_1", "rep")

BS = 128
CHUNK = 8
SUBLANES = 8
F32 = jnp.float32
BF16 = jnp.bfloat16
F16 = jnp.float16
VMEM = pltpu.VMEM
SMEM = pltpu.SMEM


def whole(space=VMEM):
    return pl.BlockSpec(memory_space=space)


def near(array):
    return pltpu.with_memory_space_constraint(array, VMEM)


def select_kernel(names, place, table, out):
    reps, named = names.shape
    for peer in range(reps):
        back = lax.rem(place[0] + reps - peer, reps)
        for t in range(named):
            out[peer, t] = table[names[back, t]]


def gram_kernel(rows, gram):
    reps, per_owner, width, _ = rows.shape
    total = jnp.zeros(gram.shape, F32)
    for t in range(per_owner):
        total = total + lax.dot_general(
            rows[0, t],
            rows[:, t].reshape(reps * width, BS),
            (((1,), (1,)), ((), ())),
            preferred_element_type=F32,
        )
    gram[...] = total


def fit_kernel(grams, rows, fitted):
    reps, per_owner, width, _ = rows.shape
    gram = grams[0]
    for source in range(1, grams.shape[0]):
        gram = gram + grams[source]
    rest = gram * gram
    pieces = []
    for _ in range(3):
        piece = rest.astype(BF16)
        rest = rest - piece.astype(F32)
        pieces.append(piece)
    for t in range(per_owner):
        block = rows[:, t].reshape(reps * width, BS)
        value = jnp.dot(pieces[2], block, preferred_element_type=F32)
        value = value + jnp.dot(pieces[1], block, preferred_element_type=F32)
        fitted[t] = value + jnp.dot(pieces[0], block, preferred_element_type=F32)


def fetch(source, target, arrived, piece):
    held = 2 * CHUNK
    per_slot = BS // held
    slot = piece // per_slot
    rows = pl.ds((piece - slot * per_slot) * held, held)
    return pltpu.make_async_copy(source.at[slot, rows], target.at[slot, rows], arrived.at[piece])


def contract_kernel(
    triples, count, x_far, sel, out,
    x, arrived, fac, low, mid, lower_a, middle_a, lower_b, middle_b, y1, y2, y3,
):
    slots = x.shape[0]
    reps, _, width, _ = sel.shape
    rank = reps * width
    per_slot = BS // CHUNK
    chunks = slots * per_slot
    pieces = chunks // 2
    for piece in range(pieces):
        fetch(x_far, x, arrived, piece).start()
    for slot in range(slots):
        for side in range(3):
            turned = sel[:, slot * 3 + side].reshape(rank, BS).astype(F32).T
            if side < 2:
                fac[slot, side] = turned
            if side == 2:
                low[slot] = turned.astype(BF16)
            if side == 1:
                mid[slot] = turned.astype(BF16)
    y2[...] = jnp.zeros_like(y2)
    y3[...] = jnp.zeros_like(y3)

    def multiply(chunk, lower_s, middle_s):
        slot = chunk // per_slot
        row0 = pl.multiple_of(lax.rem(chunk, per_slot) * CHUNK, CHUNK)
        blocks = x[slot, pl.ds(row0, CHUNK)]
        lower_s[...] = jnp.dot(
            blocks.reshape(CHUNK * BS, BS), low[slot], preferred_element_type=F32
        ).reshape(CHUNK, BS, rank)
        turned = jnp.concatenate([blocks[a].T for a in range(CHUNK)], axis=0)
        middle_s[...] = jnp.dot(turned, mid[slot], preferred_element_type=F32).reshape(
            CHUNK, BS, rank
        )

    def reduce(chunk, lower_s, middle_s):
        slot = chunk // per_slot
        row0 = pl.multiple_of(lax.rem(chunk, per_slot) * CHUNK, CHUNK)
        for half in range(rank // BS):
            cols = slice(half * BS, (half + 1) * BS)
            upper_rows = fac[slot, 0, pl.ds(row0, CHUNK), cols]
            spread = [
                jnp.broadcast_to(upper_rows[a : a + 1], (SUBLANES, BS)) for a in range(CHUNK)
            ]
            sums = [jnp.zeros((SUBLANES, BS), F32) for _ in range(CHUNK)]
            for b in range(0, BS, SUBLANES):
                rows = slice(b, b + SUBLANES)
                other = fac[slot, 1, rows, cols]
                second = y2[slot, rows, cols]
                third = y3[slot, rows, cols]
                for a in range(CHUNK):
                    value = lower_s[a, rows, cols]
                    sums[a] = sums[a] + value * other
                    second = second + value * spread[a]
                    third = third + middle_s[a, rows, cols] * spread[a]
                y2[slot, rows, cols] = second
                y3[slot, rows, cols] = third
            y1[slot, pl.ds(row0, CHUNK), cols] = jnp.concatenate(
                [jnp.sum(sums[a], axis=0, keepdims=True) for a in range(CHUNK)], axis=0
            )

    fetch(x_far, x, arrived, 0).wait()
    multiply(0, lower_a, middle_a)

    def pair(step, carry):
        @pl.when(step + 1 < pieces)
        def _():
            fetch(x_far, x, arrived, step + 1).wait()

        multiply(2 * step + 1, lower_b, middle_b)
        reduce(2 * step, lower_a, middle_a)
        multiply(jnp.minimum(2 * step + 2, chunks - 1), lower_a, middle_a)
        reduce(2 * step + 1, lower_b, middle_b)
        return carry

    lax.fori_loop(0, chunks // 2, pair, 0)

    for slot in range(slots):
        i, j, k = triples[slot, 0], triples[slot, 1], triples[slot, 2]
        upper_tie = i == j
        lower_tie = j == k
        alive = jnp.where(slot < count[0], 1.0, 0.0)
        base = jnp.where(upper_tie | lower_tie, 1.0, 2.0) * alive
        dropped = jnp.where(upper_tie & lower_tie, 0.0, base)
        for side, (value, weight) in enumerate(((y1, base), (y2, dropped), (y3, dropped))):
            out[:, slot * 3 + side] = (value[slot].T * weight).reshape(reps, width, BS)


def scatter_kernel(names, place, parts, out, total):
    reps, named = names.shape
    owners = out.shape[0]
    width = parts.shape[2]
    per_owner = total.shape[0] // owners
    total[...] = jnp.zeros_like(total)
    for peer in range(reps):
        back = lax.rem(place[0] + reps - peer, reps)
        for t in range(named):
            at = names[back, t]
            total[at] = total[at] + parts[peer, t]
    top = jnp.max(jnp.abs(total[...]), axis=(0, 1), keepdims=True)[0]
    top = jnp.max(top, axis=1, keepdims=True)
    power = jnp.clip(14.0 - jnp.ceil(jnp.log2(jnp.maximum(top, 1e-36))), -100.0, 100.0)
    power = jnp.broadcast_to(power, (SUBLANES, BS))
    scale = jnp.exp2(power)
    scale = jnp.concatenate([scale] * (width // SUBLANES), axis=0)
    for owner in range(owners):
        for t in range(per_owner):
            out[owner, t * width : (t + 1) * width] = total[owner * per_owner + t] * scale
        out[owner, per_owner * width :] = power


def moved(array, axis, shift):
    peers = lax.axis_size(axis)
    return lax.ppermute(array, axis, [(i, (i + shift) % peers) for i in range(peers)])


def from_each(array, axis):
    peers = lax.axis_size(axis)
    return jnp.stack([array] + [moved(array, axis, shift) for shift in range(1, peers)])


def shards(tensor_blocks, triples, slot_count, factor):
    slots = tensor_blocks.shape[0]
    reps = lax.axis_size("rep")
    owners = lax.axis_size(BLK)
    rows, width = factor.shape
    per_owner = rows // BS
    rank = reps * width
    named = 3 * slots
    place = lax.axis_index("rep").astype(jnp.int32).reshape(1)
    own = factor.T.reshape(width, per_owner, BS).swapaxes(0, 1)

    table = lax.all_to_all(
        jnp.broadcast_to(own[None], (owners, *own.shape)), BLK, 0, 0, tiled=True
    ).reshape(owners * per_owner, width, BS)

    listed = jnp.pad(triples.reshape(1, named).astype(BF16), ((0, 15), (0, BS - named)))
    around = from_each(jnp.concatenate([own.reshape(per_owner * width, BS), listed]), "rep")
    names = around[:, per_owner * width, :named].astype(jnp.int32)
    own_rows = around[:, : per_owner * width].reshape(reps, per_owner, width, BS)
    gram = pl.pallas_call(
        gram_kernel,
        out_shape=jax.ShapeDtypeStruct((width, rank), F32),
        in_specs=[whole()],
        out_specs=whole(),
        compiler_params=pltpu.CompilerParams(vmem_limit_bytes=16 << 20),
        name="gram",
    )(own_rows)

    chosen = pl.pallas_call(
        select_kernel,
        out_shape=VMEM((reps, named, width, BS), BF16),
        in_specs=[whole(SMEM), whole(SMEM), whole()],
        out_specs=whole(),
        compiler_params=pltpu.CompilerParams(vmem_limit_bytes=16 << 20),
        name="select",
    )(names, place, near(table))
    chosen = lax.all_to_all(chosen, "rep", 0, 0, tiled=True)

    gram = from_each(gram, "blk_1").sum(0)

    parts = pl.pallas_call(
        contract_kernel,
        out_shape=VMEM((reps, named, width, BS), F32),
        in_specs=[whole(SMEM), whole(SMEM), whole(pltpu.HBM), whole()],
        out_specs=whole(),
        scratch_shapes=[
            VMEM((slots, BS, BS, BS), BF16),
            pltpu.SemaphoreType.DMA((slots * BS // (2 * CHUNK),)),
            VMEM((slots, 2, BS, rank), F32),
            VMEM((slots, BS, rank), BF16),
            VMEM((slots, BS, rank), BF16),
            VMEM((CHUNK, BS, rank), F32),
            VMEM((CHUNK, BS, rank), F32),
            VMEM((CHUNK, BS, rank), F32),
            VMEM((CHUNK, BS, rank), F32),
            VMEM((slots, BS, rank), F32),
            VMEM((slots, BS, rank), F32),
            VMEM((slots, BS, rank), F32),
        ],
        compiler_params=pltpu.CompilerParams(vmem_limit_bytes=32 << 20),
        name="contract",
    )(triples, slot_count, tensor_blocks, near(chosen))
    parts = lax.all_to_all(parts, "rep", 0, 0, tiled=True)

    fitted = pl.pallas_call(
        fit_kernel,
        out_shape=jax.ShapeDtypeStruct((per_owner, width, BS), F32),
        in_specs=[whole(), whole()],
        out_specs=whole(),
        compiler_params=pltpu.CompilerParams(vmem_limit_bytes=16 << 20),
        name="fit",
    )(from_each(gram, "blk_0"), own_rows)

    held = per_owner * width
    scaled = pl.pallas_call(
        scatter_kernel,
        out_shape=VMEM((owners, held + SUBLANES, BS), F32),
        in_specs=[whole(SMEM), whole(SMEM), whole()],
        out_specs=whole(),
        scratch_shapes=[VMEM((owners * per_owner, width, BS), F32)],
        compiler_params=pltpu.CompilerParams(vmem_limit_bytes=16 << 20),
        name="scatter",
    )(names, place, near(parts))
    arrived = lax.all_to_all(scaled.astype(F16), BLK, 0, 0, tiled=True).astype(F32)
    moment = (arrived[:, :held] * jnp.exp2(-arrived[:, held:, :1][:, :1])).sum(0)
    gradient = fitted - moment.reshape(per_owner, width, BS)
    return gradient.swapaxes(0, 1).reshape(width, rows).T


def solution(mesh):
    split = Mesh(mesh.devices.reshape(8, 4, mesh.shape["rep"]), ("blk_0", "blk_1", "rep"))
    in_specs = (P(BLK_REP, None, None, None), P(BLK_REP, None), P(BLK_REP), P(BLK, "rep"))
    out_specs = P(BLK, "rep")
    return jax.shard_map(
        shards, mesh=split, in_specs=in_specs, out_specs=out_specs, check_vma=False
    )
```

```python
import jax
import jax.numpy as jnp
from jax import lax
from jax.experimental import pallas as pl
from jax.experimental.pallas import tpu as pltpu
from jax.sharding import Mesh
from jax.sharding import PartitionSpec as P


BLK = ("blk_0", "blk_1")
BLK_REP = ("blk_0", "blk_1", "rep")

BS = 128
CHUNK = 8
SUBLANES = 8
F32 = jnp.float32
BF16 = jnp.bfloat16
F16 = jnp.float16
VMEM = pltpu.VMEM
SMEM = pltpu.SMEM


def whole(space=VMEM):
    return pl.BlockSpec(memory_space=space)


def near(array):
    return pltpu.with_memory_space_constraint(array, VMEM)


def select_kernel(names, place, table, out):
    reps, named = names.shape
    for peer in range(reps):
        back = lax.rem(place[0] + reps - peer, reps)
        for t in range(named):
            out[peer, t] = table[names[back, t]]


def gram_kernel(rows, gram):
    reps, per_owner, width, _ = rows.shape
    total = jnp.zeros(gram.shape, F32)
    for t in range(per_owner):
        total = total + lax.dot_general(
            rows[0, t],
            rows[:, t].reshape(reps * width, BS),
            (((1,), (1,)), ((), ())),
            preferred_element_type=F32,
        )
    gram[...] = total


def fit_kernel(grams, rows, fitted):
    reps, per_owner, width, _ = rows.shape
    gram = grams[0]
    for source in range(1, grams.shape[0]):
        gram = gram + grams[source]
    rest = gram * gram
    pieces = []
    for _ in range(3):
        piece = rest.astype(BF16)
        rest = rest - piece.astype(F32)
        pieces.append(piece)
    for t in range(per_owner):
        block = rows[:, t].reshape(reps * width, BS)
        value = jnp.dot(pieces[2], block, preferred_element_type=F32)
        value = value + jnp.dot(pieces[1], block, preferred_element_type=F32)
        fitted[t] = value + jnp.dot(pieces[0], block, preferred_element_type=F32)


def fetch(source, target, arrived, piece):
    held = 2 * CHUNK
    per_slot = BS // held
    slot = piece // per_slot
    rows = pl.ds((piece - slot * per_slot) * held, held)
    return pltpu.make_async_copy(source.at[slot, rows], target.at[slot, rows], arrived.at[piece])


def contract_kernel(
    triples, count, x_far, sel, out,
    x, arrived, fac, low, mid, lower_a, middle_a, lower_b, middle_b, y1, y2, y3,
):
    slots = x.shape[0]
    reps, _, width, _ = sel.shape
    rank = reps * width
    per_slot = BS // CHUNK
    chunks = slots * per_slot
    pieces = chunks // 2
    for piece in range(pieces):
        fetch(x_far, x, arrived, piece).start()
    for slot in range(slots):
        for side in range(3):
            turned = sel[:, slot * 3 + side].reshape(rank, BS).astype(F32).T
            if side < 2:
                fac[slot, side] = turned
            if side == 2:
                low[slot] = turned.astype(BF16)
            if side == 1:
                mid[slot] = turned.astype(BF16)
    y2[...] = jnp.zeros_like(y2)
    y3[...] = jnp.zeros_like(y3)

    def multiply(chunk, lower_s, middle_s):
        slot = chunk // per_slot
        row0 = pl.multiple_of(lax.rem(chunk, per_slot) * CHUNK, CHUNK)
        blocks = x[slot, pl.ds(row0, CHUNK)]
        lower_s[...] = jnp.dot(
            blocks.reshape(CHUNK * BS, BS), low[slot], preferred_element_type=F32
        ).reshape(CHUNK, BS, rank)
        turned = jnp.concatenate([blocks[a].T for a in range(CHUNK)], axis=0)
        middle_s[...] = jnp.dot(turned, mid[slot], preferred_element_type=F32).reshape(
            CHUNK, BS, rank
        )

    def reduce(chunk, lower_s, middle_s):
        slot = chunk // per_slot
        row0 = pl.multiple_of(lax.rem(chunk, per_slot) * CHUNK, CHUNK)
        for half in range(rank // BS):
            cols = slice(half * BS, (half + 1) * BS)
            upper_rows = fac[slot, 0, pl.ds(row0, CHUNK), cols]
            spread = [
                jnp.broadcast_to(upper_rows[a : a + 1], (SUBLANES, BS)) for a in range(CHUNK)
            ]
            sums = [jnp.zeros((SUBLANES, BS), F32) for _ in range(CHUNK)]
            for b in range(0, BS, SUBLANES):
                rows = slice(b, b + SUBLANES)
                other = fac[slot, 1, rows, cols]
                second = y2[slot, rows, cols]
                third = y3[slot, rows, cols]
                for a in range(CHUNK):
                    value = lower_s[a, rows, cols]
                    sums[a] = sums[a] + value * other
                    second = second + value * spread[a]
                    third = third + middle_s[a, rows, cols] * spread[a]
                y2[slot, rows, cols] = second
                y3[slot, rows, cols] = third
            y1[slot, pl.ds(row0, CHUNK), cols] = jnp.concatenate(
                [jnp.sum(sums[a], axis=0, keepdims=True) for a in range(CHUNK)], axis=0
            )

    fetch(x_far, x, arrived, 0).wait()
    multiply(0, lower_a, middle_a)

    def pair(step, carry):
        @pl.when(step + 1 < pieces)
        def _():
            fetch(x_far, x, arrived, step + 1).wait()

        multiply(2 * step + 1, lower_b, middle_b)
        reduce(2 * step, lower_a, middle_a)
        multiply(jnp.minimum(2 * step + 2, chunks - 1), lower_a, middle_a)
        reduce(2 * step + 1, lower_b, middle_b)
        return carry

    lax.fori_loop(0, chunks // 2, pair, 0)

    for slot in range(slots):
        i, j, k = triples[slot, 0], triples[slot, 1], triples[slot, 2]
        upper_tie = i == j
        lower_tie = j == k
        alive = jnp.where(slot < count[0], 1.0, 0.0)
        base = jnp.where(upper_tie | lower_tie, 1.0, 2.0) * alive
        dropped = jnp.where(upper_tie & lower_tie, 0.0, base)
        for side, (value, weight) in enumerate(((y1, base), (y2, dropped), (y3, dropped))):
            out[:, slot * 3 + side] = (value[slot].T * weight).reshape(reps, width, BS)


def scatter_kernel(names, place, parts, out, total):
    reps, named = names.shape
    owners = out.shape[0]
    width = parts.shape[2]
    per_owner = total.shape[0] // owners
    total[...] = jnp.zeros_like(total)
    for peer in range(reps):
        back = lax.rem(place[0] + reps - peer, reps)
        for t in range(named):
            at = names[back, t]
            total[at] = total[at] + parts[peer, t]
    top = jnp.max(jnp.abs(total[...]), axis=(0, 1), keepdims=True)[0]
    top = jnp.max(top, axis=1, keepdims=True)
    power = jnp.clip(14.0 - jnp.ceil(jnp.log2(jnp.maximum(top, 1e-36))), -100.0, 100.0)
    power = jnp.broadcast_to(power, (SUBLANES, BS))
    scale = jnp.exp2(power)
    scale = jnp.concatenate([scale] * (width // SUBLANES), axis=0)
    for owner in range(owners):
        for t in range(per_owner):
            out[owner, t * width : (t + 1) * width] = total[owner * per_owner + t] * scale
        out[owner, per_owner * width :] = power


def moved(array, axis, shift):
    peers = lax.axis_size(axis)
    return lax.ppermute(array, axis, [(i, (i + shift) % peers) for i in range(peers)])


def from_each(array, axis):
    peers = lax.axis_size(axis)
    return jnp.stack([array] + [moved(array, axis, shift) for shift in range(1, peers)])


def shards(tensor_blocks, triples, slot_count, factor):
    slots = tensor_blocks.shape[0]
    reps = lax.axis_size("rep")
    owners = lax.axis_size(BLK)
    rows, width = factor.shape
    per_owner = rows // BS
    rank = reps * width
    named = 3 * slots
    place = lax.axis_index("rep").astype(jnp.int32).reshape(1)
    own = factor.T.reshape(width, per_owner, BS).swapaxes(0, 1)

    table = lax.all_to_all(
        jnp.broadcast_to(own[None], (owners, *own.shape)), BLK, 0, 0, tiled=True
    ).reshape(owners * per_owner, width, BS)

    listed = jnp.pad(triples.reshape(1, named).astype(BF16), ((0, 15), (0, BS - named)))
    around = from_each(jnp.concatenate([own.reshape(per_owner * width, BS), listed]), "rep")
    names = around[:, per_owner * width, :named].astype(jnp.int32)
    own_rows = around[:, : per_owner * width].reshape(reps, per_owner, width, BS)
    gram = pl.pallas_call(
        gram_kernel,
        out_shape=jax.ShapeDtypeStruct((width, rank), F32),
        in_specs=[whole()],
        out_specs=whole(),
        compiler_params=pltpu.CompilerParams(vmem_limit_bytes=16 << 20),
        name="gram",
    )(own_rows)

    chosen = pl.pallas_call(
        select_kernel,
        out_shape=VMEM((reps, named, width, BS), BF16),
        in_specs=[whole(SMEM), whole(SMEM), whole()],
        out_specs=whole(),
        compiler_params=pltpu.CompilerParams(vmem_limit_bytes=16 << 20),
        name="select",
    )(names, place, near(table))
    chosen = lax.all_to_all(chosen, "rep", 0, 0, tiled=True)

    gram = from_each(gram, "blk_1").sum(0)

    parts = pl.pallas_call(
        contract_kernel,
        out_shape=VMEM((reps, named, width, BS), F32),
        in_specs=[whole(SMEM), whole(SMEM), whole(pltpu.HBM), whole()],
        out_specs=whole(),
        scratch_shapes=[
            VMEM((slots, BS, BS, BS), BF16),
            pltpu.SemaphoreType.DMA((slots * BS // (2 * CHUNK),)),
            VMEM((slots, 2, BS, rank), F32),
            VMEM((slots, BS, rank), BF16),
            VMEM((slots, BS, rank), BF16),
            VMEM((CHUNK, BS, rank), F32),
            VMEM((CHUNK, BS, rank), F32),
            VMEM((CHUNK, BS, rank), F32),
            VMEM((CHUNK, BS, rank), F32),
            VMEM((slots, BS, rank), F32),
            VMEM((slots, BS, rank), F32),
            VMEM((slots, BS, rank), F32),
        ],
        compiler_params=pltpu.CompilerParams(vmem_limit_bytes=32 << 20),
        name="contract",
    )(
        triples,
        slot_count,
        pltpu.with_memory_space_constraint(tensor_blocks, pltpu.HBM),
        near(chosen),
    )
    parts = lax.all_to_all(parts, "rep", 0, 0, tiled=True)

    grams = from_each(gram, "blk_0")
    fitted = pl.pallas_call(
        fit_kernel,
        out_shape=jax.ShapeDtypeStruct((per_owner, width, BS), F32),
        in_specs=[whole(), whole()],
        out_specs=whole(),
        compiler_params=pltpu.CompilerParams(vmem_limit_bytes=16 << 20),
        name="fit",
    )(grams, own_rows)

    held = per_owner * width
    scaled = pl.pallas_call(
        scatter_kernel,
        out_shape=VMEM((owners, held + SUBLANES, BS), F32),
        in_specs=[whole(SMEM), whole(SMEM), whole()],
        out_specs=whole(),
        scratch_shapes=[VMEM((owners * per_owner, width, BS), F32)],
        compiler_params=pltpu.CompilerParams(vmem_limit_bytes=16 << 20),
        name="scatter",
    )(names, place, near(parts))
    arrived = lax.all_to_all(scaled.astype(F16), BLK, 0, 0, tiled=True)
    arrived = arrived.astype(F32)
    moment = (arrived[:, :held] * jnp.exp2(-arrived[:, held:, :1][:, :1])).sum(0)
    gradient = fitted - moment.reshape(per_owner, width, BS)
    return gradient.swapaxes(0, 1).reshape(width, rows).T


def solution(mesh):
    split = Mesh(mesh.devices.reshape(8, 4, mesh.shape["rep"]), ("blk_0", "blk_1", "rep"))
    in_specs = (P(BLK_REP, None, None, None), P(BLK_REP, None), P(BLK_REP), P(BLK, "rep"))
    out_specs = P(BLK, "rep")
    return jax.shard_map(
        shards, mesh=split, in_specs=in_specs, out_specs=out_specs, check_vma=False
    )
```

```python
import jax
import jax.numpy as jnp
from jax import lax
from jax.experimental import pallas as pl
from jax.experimental.pallas import tpu as pltpu
from jax.sharding import Mesh
from jax.sharding import PartitionSpec as P


BLK = ("blk_0", "blk_1")
BLK_REP = ("blk_0", "blk_1", "rep")

BS = 128
CHUNK = 8
SUBLANES = 8
STEP = 4
AHEAD = 3
F32 = jnp.float32
BF16 = jnp.bfloat16
F16 = jnp.float16
VMEM = pltpu.VMEM
SMEM = pltpu.SMEM


def whole(space=VMEM):
    return pl.BlockSpec(memory_space=space)


def near(array):
    return pltpu.with_memory_space_constraint(array, VMEM)


def select_kernel(names, place, table, out):
    reps, named = names.shape
    for peer in range(reps):
        back = lax.rem(place[0] + reps - peer, reps)
        for t in range(named):
            out[peer, t] = table[names[back, t]]


def gram_kernel(rows, gram):
    reps, per_owner, width, _ = rows.shape
    total = jnp.zeros(gram.shape, F32)
    for t in range(per_owner):
        total = total + lax.dot_general(
            rows[0, t],
            rows[:, t].reshape(reps * width, BS),
            (((1,), (1,)), ((), ())),
            preferred_element_type=F32,
        )
    gram[...] = total


def fit_kernel(gram, rows, fitted):
    reps, per_owner, width, _ = rows.shape
    rest = gram[...] * gram[...]
    pieces = []
    for _ in range(3):
        piece = rest.astype(BF16)
        rest = rest - piece.astype(F32)
        pieces.append(piece)
    for t in range(per_owner):
        block = rows[:, t].reshape(reps * width, BS)
        value = jnp.dot(pieces[2], block, preferred_element_type=F32)
        value = value + jnp.dot(pieces[1], block, preferred_element_type=F32)
        fitted[t] = value + jnp.dot(pieces[0], block, preferred_element_type=F32)


def fetch(source, target, arrived, piece):
    held = STEP * CHUNK
    per_slot = BS // held
    slot = piece // per_slot
    rows = pl.ds((piece - slot * per_slot) * held, held)
    return pltpu.make_async_copy(source.at[slot, rows], target.at[slot, rows], arrived.at[piece])


def contract_kernel(
    triples, count, x_far, sel, out,
    x, arrived, fac, low, mid, lower_a, middle_a, lower_b, middle_b, y1, y2, y3,
):
    slots = x.shape[0]
    reps, _, width, _ = sel.shape
    rank = reps * width
    per_slot = BS // CHUNK
    chunks = slots * per_slot
    pieces = chunks // STEP
    for piece in range(min(AHEAD, pieces)):
        fetch(x_far, x, arrived, piece).start()
    for slot in range(slots):
        for side in range(3):
            turned = sel[:, slot * 3 + side].reshape(rank, BS).astype(F32).T
            if side < 2:
                fac[slot, side] = turned
            if side == 2:
                low[slot] = turned.astype(BF16)
            if side == 1:
                mid[slot] = turned.astype(BF16)
    y2[...] = jnp.zeros_like(y2)
    y3[...] = jnp.zeros_like(y3)

    def multiply(chunk, lower_s, middle_s):
        slot = chunk // per_slot
        row0 = pl.multiple_of(lax.rem(chunk, per_slot) * CHUNK, CHUNK)
        blocks = x[slot, pl.ds(row0, CHUNK)]
        lower_s[...] = jnp.dot(
            blocks.reshape(CHUNK * BS, BS), low[slot], preferred_element_type=F32
        ).reshape(CHUNK, BS, rank)
        turned = jnp.concatenate([blocks[a].T for a in range(CHUNK)], axis=0)
        middle_s[...] = jnp.dot(turned, mid[slot], preferred_element_type=F32).reshape(
            CHUNK, BS, rank
        )

    def reduce(chunk, lower_s, middle_s):
        slot = chunk // per_slot
        row0 = pl.multiple_of(lax.rem(chunk, per_slot) * CHUNK, CHUNK)
        for half in range(rank // BS):
            cols = slice(half * BS, (half + 1) * BS)
            upper_rows = fac[slot, 0, pl.ds(row0, CHUNK), cols]
            spread = [
                jnp.broadcast_to(upper_rows[a : a + 1], (SUBLANES, BS)) for a in range(CHUNK)
            ]
            sums = [jnp.zeros((SUBLANES, BS), F32) for _ in range(CHUNK)]
            for b in range(0, BS, SUBLANES):
                rows = slice(b, b + SUBLANES)
                other = fac[slot, 1, rows, cols]
                second = y2[slot, rows, cols]
                third = y3[slot, rows, cols]
                for a in range(CHUNK):
                    value = lower_s[a, rows, cols]
                    sums[a] = sums[a] + value * other
                    second = second + value * spread[a]
                    third = third + middle_s[a, rows, cols] * spread[a]
                y2[slot, rows, cols] = second
                y3[slot, rows, cols] = third
            y1[slot, pl.ds(row0, CHUNK), cols] = jnp.concatenate(
                [jnp.sum(sums[a], axis=0, keepdims=True) for a in range(CHUNK)], axis=0
            )

    fetch(x_far, x, arrived, 0).wait()
    multiply(0, lower_a, middle_a)

    def several(step, carry):
        @pl.when(step + AHEAD < pieces)
        def _():
            fetch(x_far, x, arrived, step + AHEAD).start()

        @pl.when(step + 1 < pieces)
        def _():
            fetch(x_far, x, arrived, step + 1).wait()

        first = step * STEP
        for n in range(STEP):
            here, there = (lower_a, middle_a), (lower_b, middle_b)
            if n % 2:
                here, there = there, here
            multiply(jnp.minimum(first + n + 1, chunks - 1), *there)
            reduce(first + n, *here)
        return carry

    lax.fori_loop(0, pieces, several, 0)

    for slot in range(slots):
        i, j, k = triples[slot, 0], triples[slot, 1], triples[slot, 2]
        upper_tie = i == j
        lower_tie = j == k
        alive = jnp.where(slot < count[0], 1.0, 0.0)
        base = jnp.where(upper_tie | lower_tie, 1.0, 2.0) * alive
        dropped = jnp.where(upper_tie & lower_tie, 0.0, base)
        for side, (value, weight) in enumerate(((y1, base), (y2, dropped), (y3, dropped))):
            out[:, slot * 3 + side] = (value[slot].T * weight).reshape(reps, width, BS)


def scatter_kernel(names, place, parts, out, total):
    reps, named = names.shape
    owners = out.shape[0]
    width = parts.shape[2]
    per_owner = total.shape[0] // owners
    total[...] = jnp.zeros_like(total)
    for peer in range(reps):
        back = lax.rem(place[0] + reps - peer, reps)
        for t in range(named):
            at = names[back, t]
            total[at] = total[at] + parts[peer, t]
    top = jnp.max(jnp.abs(total[...]), axis=(0, 1), keepdims=True)[0]
    top = jnp.max(top, axis=1, keepdims=True)
    power = jnp.clip(14.0 - jnp.ceil(jnp.log2(jnp.maximum(top, 1e-36))), -100.0, 100.0)
    power = jnp.broadcast_to(power, (SUBLANES, BS))
    scale = jnp.exp2(power)
    scale = jnp.concatenate([scale] * (width // SUBLANES), axis=0)
    for owner in range(owners):
        for t in range(per_owner):
            out[owner, t * width : (t + 1) * width] = total[owner * per_owner + t] * scale
        out[owner, per_owner * width :] = power


def moved(array, axis, shift):
    peers = lax.axis_size(axis)
    return lax.ppermute(array, axis, [(i, (i + shift) % peers) for i in range(peers)])


def from_each(array, axis):
    peers = lax.axis_size(axis)
    return jnp.stack([array] + [moved(array, axis, shift) for shift in range(1, peers)])


def summed(array, axis):
    peers = lax.axis_size(axis)
    bit = 1
    while bit < peers:
        swap = [(i, i ^ bit) for i in range(peers)]
        array = array + lax.ppermute(array, axis, swap)
        bit *= 2
    return array


def shards(tensor_blocks, triples, slot_count, factor):
    slots = tensor_blocks.shape[0]
    reps = lax.axis_size("rep")
    owners = lax.axis_size(BLK)
    rows, width = factor.shape
    per_owner = rows // BS
    rank = reps * width
    named = 3 * slots
    place = lax.axis_index("rep").astype(jnp.int32).reshape(1)
    own = factor.T.reshape(width, per_owner, BS).swapaxes(0, 1)

    table = lax.all_to_all(
        jnp.broadcast_to(own[None], (owners, *own.shape)), BLK, 0, 0, tiled=True
    ).reshape(owners * per_owner, width, BS)

    listed = jnp.pad(triples.reshape(1, named).astype(BF16), ((0, 15), (0, BS - named)))
    around = from_each(jnp.concatenate([own.reshape(per_owner * width, BS), listed]), "rep")
    names = around[:, per_owner * width, :named].astype(jnp.int32)
    own_rows = around[:, : per_owner * width].reshape(reps, per_owner, width, BS)
    gram = pl.pallas_call(
        gram_kernel,
        out_shape=jax.ShapeDtypeStruct((width, rank), F32),
        in_specs=[whole()],
        out_specs=whole(),
        compiler_params=pltpu.CompilerParams(vmem_limit_bytes=16 << 20),
        name="gram",
    )(own_rows)

    chosen = pl.pallas_call(
        select_kernel,
        out_shape=VMEM((reps, named, width, BS), BF16),
        in_specs=[whole(SMEM), whole(SMEM), whole()],
        out_specs=whole(),
        compiler_params=pltpu.CompilerParams(vmem_limit_bytes=16 << 20),
        name="select",
    )(names, place, near(table))
    chosen = lax.all_to_all(chosen, "rep", 0, 0, tiled=True)

    gram = summed(gram, "blk_1")

    parts = pl.pallas_call(
        contract_kernel,
        out_shape=VMEM((reps, named, width, BS), F32),
        in_specs=[whole(SMEM), whole(SMEM), whole(pltpu.HBM), whole()],
        out_specs=whole(),
        scratch_shapes=[
            VMEM((slots, BS, BS, BS), BF16),
            pltpu.SemaphoreType.DMA((slots * BS // (STEP * CHUNK),)),
            VMEM((slots, 2, BS, rank), F32),
            VMEM((slots, BS, rank), BF16),
            VMEM((slots, BS, rank), BF16),
            VMEM((CHUNK, BS, rank), F32),
            VMEM((CHUNK, BS, rank), F32),
            VMEM((CHUNK, BS, rank), F32),
            VMEM((CHUNK, BS, rank), F32),
            VMEM((slots, BS, rank), F32),
            VMEM((slots, BS, rank), F32),
            VMEM((slots, BS, rank), F32),
        ],
        compiler_params=pltpu.CompilerParams(vmem_limit_bytes=32 << 20),
        name="contract",
    )(
        triples,
        slot_count,
        pltpu.with_memory_space_constraint(tensor_blocks, pltpu.HBM),
        near(chosen),
    )
    parts = lax.all_to_all(parts, "rep", 0, 0, tiled=True)

    gram = summed(gram, "blk_0")
    fitted = pl.pallas_call(
        fit_kernel,
        out_shape=jax.ShapeDtypeStruct((per_owner, width, BS), F32),
        in_specs=[whole(), whole()],
        out_specs=whole(),
        compiler_params=pltpu.CompilerParams(vmem_limit_bytes=16 << 20),
        name="fit",
    )(gram, own_rows)

    held = per_owner * width
    scaled = pl.pallas_call(
        scatter_kernel,
        out_shape=VMEM((owners, held + SUBLANES, BS), F32),
        in_specs=[whole(SMEM), whole(SMEM), whole()],
        out_specs=whole(),
        scratch_shapes=[VMEM((owners * per_owner, width, BS), F32)],
        compiler_params=pltpu.CompilerParams(vmem_limit_bytes=16 << 20),
        name="scatter",
    )(names, place, near(parts))
    arrived = lax.all_to_all(scaled.astype(F16), BLK, 0, 0, tiled=True)
    arrived = arrived.astype(F32)
    moment = (arrived[:, :held] * jnp.exp2(-arrived[:, held:, :1][:, :1])).sum(0)
    gradient = fitted - moment.reshape(per_owner, width, BS)
    return gradient.swapaxes(0, 1).reshape(width, rows).T


def solution(mesh):
    split = Mesh(mesh.devices.reshape(8, 4, mesh.shape["rep"]), ("blk_0", "blk_1", "rep"))
    in_specs = (P(BLK_REP, None, None, None), P(BLK_REP, None), P(BLK_REP), P(BLK, "rep"))
    out_specs = P(BLK, "rep")
    return jax.shard_map(
        shards, mesh=split, in_specs=in_specs, out_specs=out_specs, check_vma=False
    )
```

```python
import jax
import jax.numpy as jnp
from jax import lax
from jax.experimental import pallas as pl
from jax.experimental.pallas import tpu as pltpu
from jax.sharding import Mesh
from jax.sharding import PartitionSpec as P


BLK = ("blk_0", "blk_1")
BLK_REP = ("blk_0", "blk_1", "rep")

BS = 128
CHUNK = 8
SUBLANES = 8
STEP = 4
AHEAD = 3
F32 = jnp.float32
BF16 = jnp.bfloat16
F16 = jnp.float16
VMEM = pltpu.VMEM
SMEM = pltpu.SMEM


def whole(space=VMEM):
    return pl.BlockSpec(memory_space=space)


def near(array):
    return pltpu.with_memory_space_constraint(array, VMEM)


def select_kernel(names, place, table, out):
    reps, named = names.shape
    for peer in range(reps):
        back = jnp.bitwise_xor(place[0], peer)
        for t in range(named):
            out[peer, t] = table[names[back, t]]


def gram_kernel(rows, gram):
    reps, per_owner, width, _ = rows.shape
    total = jnp.zeros(gram.shape, F32)
    for t in range(per_owner):
        total = total + lax.dot_general(
            rows[0, t],
            rows[:, t].reshape(reps * width, BS),
            (((1,), (1,)), ((), ())),
            preferred_element_type=F32,
        )
    gram[...] = total


def fit_kernel(gram, rows, fitted):
    reps, per_owner, width, _ = rows.shape
    rest = gram[...] * gram[...]
    pieces = []
    for _ in range(3):
        piece = rest.astype(BF16)
        rest = rest - piece.astype(F32)
        pieces.append(piece)
    for t in range(per_owner):
        block = rows[:, t].reshape(reps * width, BS)
        value = jnp.dot(pieces[2], block, preferred_element_type=F32)
        value = value + jnp.dot(pieces[1], block, preferred_element_type=F32)
        fitted[t] = value + jnp.dot(pieces[0], block, preferred_element_type=F32)


def fetch(source, target, arrived, piece):
    held = STEP * CHUNK
    per_slot = BS // held
    slot = piece // per_slot
    rows = pl.ds((piece - slot * per_slot) * held, held)
    return pltpu.make_async_copy(source.at[slot, rows], target.at[slot, rows], arrived.at[piece])


def contract_kernel(
    triples, count, x_far, sel, out,
    x, arrived, fac, low, mid, lower_a, middle_a, lower_b, middle_b, y1, y2, y3,
):
    slots = x.shape[0]
    reps, _, width, _ = sel.shape
    rank = reps * width
    per_slot = BS // CHUNK
    chunks = slots * per_slot
    pieces = chunks // STEP
    for piece in range(min(AHEAD, pieces)):
        fetch(x_far, x, arrived, piece).start()
    for slot in range(slots):
        for side in range(3):
            turned = sel[:, slot * 3 + side].reshape(rank, BS).astype(F32).T
            if side < 2:
                fac[slot, side] = turned
            if side == 2:
                low[slot] = turned.astype(BF16)
            if side == 1:
                mid[slot] = turned.astype(BF16)
    y2[...] = jnp.zeros_like(y2)
    y3[...] = jnp.zeros_like(y3)

    def multiply(chunk, lower_s, middle_s):
        slot = chunk // per_slot
        row0 = pl.multiple_of(lax.rem(chunk, per_slot) * CHUNK, CHUNK)
        blocks = x[slot, pl.ds(row0, CHUNK)]
        lower_s[...] = jnp.dot(
            blocks.reshape(CHUNK * BS, BS), low[slot], preferred_element_type=F32
        ).reshape(CHUNK, BS, rank)
        turned = jnp.concatenate([blocks[a].T for a in range(CHUNK)], axis=0)
        middle_s[...] = jnp.dot(turned, mid[slot], preferred_element_type=F32).reshape(
            CHUNK, BS, rank
        )

    def reduce(chunk, lower_s, middle_s):
        slot = chunk // per_slot
        row0 = pl.multiple_of(lax.rem(chunk, per_slot) * CHUNK, CHUNK)
        for half in range(rank // BS):
            cols = slice(half * BS, (half + 1) * BS)
            upper_rows = fac[slot, 0, pl.ds(row0, CHUNK), cols]
            spread = [
                jnp.broadcast_to(upper_rows[a : a + 1], (SUBLANES, BS)) for a in range(CHUNK)
            ]
            sums = [jnp.zeros((SUBLANES, BS), F32) for _ in range(CHUNK)]
            for b in range(0, BS, SUBLANES):
                rows = slice(b, b + SUBLANES)
                other = fac[slot, 1, rows, cols]
                second = y2[slot, rows, cols]
                third = y3[slot, rows, cols]
                for a in range(CHUNK):
                    value = lower_s[a, rows, cols]
                    sums[a] = sums[a] + value * other
                    second = second + value * spread[a]
                    third = third + middle_s[a, rows, cols] * spread[a]
                y2[slot, rows, cols] = second
                y3[slot, rows, cols] = third
            y1[slot, pl.ds(row0, CHUNK), cols] = jnp.concatenate(
                [jnp.sum(sums[a], axis=0, keepdims=True) for a in range(CHUNK)], axis=0
            )

    fetch(x_far, x, arrived, 0).wait()
    multiply(0, lower_a, middle_a)

    def several(step, carry):
        @pl.when(step + AHEAD < pieces)
        def _():
            fetch(x_far, x, arrived, step + AHEAD).start()

        @pl.when(step + 1 < pieces)
        def _():
            fetch(x_far, x, arrived, step + 1).wait()

        first = step * STEP
        for n in range(STEP):
            here, there = (lower_a, middle_a), (lower_b, middle_b)
            if n % 2:
                here, there = there, here
            multiply(jnp.minimum(first + n + 1, chunks - 1), *there)
            reduce(first + n, *here)
        return carry

    lax.fori_loop(0, pieces, several, 0)

    scaled = []
    top = jnp.zeros((1, 1), F32)
    for slot in range(slots):
        i, j, k = triples[slot, 0], triples[slot, 1], triples[slot, 2]
        upper_tie = i == j
        lower_tie = j == k
        alive = jnp.where(slot < count[0], 1.0, 0.0)
        base = jnp.where(upper_tie | lower_tie, 1.0, 2.0) * alive
        dropped = jnp.where(upper_tie & lower_tie, 0.0, base)
        for value, weight in ((y1, base), (y2, dropped), (y3, dropped)):
            scaled.append((value, slot, weight))
            top = jnp.maximum(top, top_of(value[slot]) * weight)
    power = power_of(top)
    scale = stretched(jnp.exp2(power), rank)
    for t, (value, slot, weight) in enumerate(scaled):
        out[:, t * width : (t + 1) * width] = (value[slot].T * (scale * weight)).reshape(
            reps, width, BS
        )
    for peer in range(reps):
        out[peer, len(scaled) * width :] = power


def power_of(top):
    power = 14.0 - jnp.ceil(jnp.log2(jnp.maximum(top, 1e-36)))
    return jnp.broadcast_to(jnp.clip(power, -120.0, 120.0), (SUBLANES, BS))


def stretched(row, count):
    return jnp.concatenate([row] * (count // SUBLANES), axis=0)


def top_of(value):
    return jnp.max(jnp.max(jnp.abs(value), axis=0, keepdims=True), axis=1, keepdims=True)


def scatter_kernel(names, place, parts, out, total):
    reps, named = names.shape
    owners = out.shape[0]
    per_owner = total.shape[0] // owners
    width = total.shape[1]
    total[...] = jnp.zeros_like(total)
    for peer in range(reps):
        back = jnp.bitwise_xor(place[0], peer)
        undo = stretched(jnp.exp2(-parts[peer, named * width :]), width)
        for t in range(named):
            at = names[back, t]
            total[at] = total[at] + parts[peer, t * width : (t + 1) * width] * undo
    power = power_of(top_of(jnp.max(jnp.abs(total[...]), axis=0)))
    scale = stretched(jnp.exp2(power), width)
    for owner in range(owners):
        for t in range(per_owner):
            out[owner, t * width : (t + 1) * width] = total[owner * per_owner + t] * scale
        out[owner, per_owner * width :] = power


def swapped(array, axis, bit):
    peers = lax.axis_size(axis)
    return lax.ppermute(array, axis, [(i, i ^ bit) for i in range(peers)])


def from_each(array, axis):
    array = array[None]
    while array.shape[0] < lax.axis_size(axis):
        array = jnp.concatenate([array, swapped(array, axis, array.shape[0])])
    return array


def summed(array, axis, bits):
    for bit in bits:
        array = array + swapped(array, axis, bit)
    return array


def shards(tensor_blocks, triples, slot_count, factor):
    slots = tensor_blocks.shape[0]
    reps = lax.axis_size("rep")
    owners = lax.axis_size(BLK)
    rows, width = factor.shape
    per_owner = rows // BS
    rank = reps * width
    named = 3 * slots
    place = lax.axis_index("rep").astype(jnp.int32).reshape(1)
    own = factor.T.reshape(width, per_owner, BS).swapaxes(0, 1)

    table = lax.all_to_all(
        jnp.broadcast_to(own[None], (owners, *own.shape)), BLK, 0, 0, tiled=True
    ).reshape(owners * per_owner, width, BS)

    listed = jnp.pad(triples.reshape(1, named).astype(BF16), ((0, 15), (0, BS - named)))
    around = from_each(jnp.concatenate([own.reshape(per_owner * width, BS), listed]), "rep")
    names = around[:, per_owner * width, :named].astype(jnp.int32)
    own_rows = around[:, : per_owner * width].reshape(reps, per_owner, width, BS)
    gram = pl.pallas_call(
        gram_kernel,
        out_shape=jax.ShapeDtypeStruct((width, rank), F32),
        in_specs=[whole()],
        out_specs=whole(),
        compiler_params=pltpu.CompilerParams(vmem_limit_bytes=16 << 20),
        name="gram",
    )(own_rows)

    chosen = pl.pallas_call(
        select_kernel,
        out_shape=VMEM((reps, named, width, BS), BF16),
        in_specs=[whole(SMEM), whole(SMEM), whole()],
        out_specs=whole(),
        compiler_params=pltpu.CompilerParams(vmem_limit_bytes=16 << 20),
        name="select",
    )(names, place, near(table))
    chosen = lax.all_to_all(chosen, "rep", 0, 0, tiled=True)

    gram = summed(gram, "blk_1", (1, 2))
    gram = summed(gram, "blk_0", (4,))

    parts = pl.pallas_call(
        contract_kernel,
        out_shape=VMEM((reps, named * width + SUBLANES, BS), F32),
        in_specs=[whole(SMEM), whole(SMEM), whole(pltpu.HBM), whole()],
        out_specs=whole(),
        scratch_shapes=[
            VMEM((slots, BS, BS, BS), BF16),
            pltpu.SemaphoreType.DMA((slots * BS // (STEP * CHUNK),)),
            VMEM((slots, 2, BS, rank), F32),
            VMEM((slots, BS, rank), BF16),
            VMEM((slots, BS, rank), BF16),
            VMEM((CHUNK, BS, rank), F32),
            VMEM((CHUNK, BS, rank), F32),
            VMEM((CHUNK, BS, rank), F32),
            VMEM((CHUNK, BS, rank), F32),
            VMEM((slots, BS, rank), F32),
            VMEM((slots, BS, rank), F32),
            VMEM((slots, BS, rank), F32),
        ],
        compiler_params=pltpu.CompilerParams(vmem_limit_bytes=32 << 20),
        name="contract",
    )(
        triples,
        slot_count,
        pltpu.with_memory_space_constraint(tensor_blocks, pltpu.HBM),
        near(chosen),
    )
    parts = lax.all_to_all(parts.astype(F16), "rep", 0, 0, tiled=True)

    gram = summed(gram, "blk_0", (1, 2))
    fitted = pl.pallas_call(
        fit_kernel,
        out_shape=jax.ShapeDtypeStruct((per_owner, width, BS), F32),
        in_specs=[whole(), whole()],
        out_specs=whole(),
        compiler_params=pltpu.CompilerParams(vmem_limit_bytes=16 << 20),
        name="fit",
    )(gram, own_rows)

    held = per_owner * width
    scaled = pl.pallas_call(
        scatter_kernel,
        out_shape=VMEM((owners, held + SUBLANES, BS), F32),
        in_specs=[whole(SMEM), whole(SMEM), whole()],
        out_specs=whole(),
        scratch_shapes=[VMEM((owners * per_owner, width, BS), F32)],
        compiler_params=pltpu.CompilerParams(vmem_limit_bytes=16 << 20),
        name="scatter",
    )(names, place, near(parts.astype(F32)))
    arrived = lax.all_to_all(scaled.astype(F16), BLK, 0, 0, tiled=True)
    arrived = arrived.astype(F32)
    moment = (arrived[:, :held] * jnp.exp2(-arrived[:, held:, :1][:, :1])).sum(0)
    gradient = fitted - moment.reshape(per_owner, width, BS)
    return gradient.swapaxes(0, 1).reshape(width, rows).T


def solution(mesh):
    split = Mesh(mesh.devices.reshape(8, 4, mesh.shape["rep"]), ("blk_0", "blk_1", "rep"))
    in_specs = (P(BLK_REP, None, None, None), P(BLK_REP, None), P(BLK_REP), P(BLK, "rep"))
    out_specs = P(BLK, "rep")
    return jax.shard_map(
        shards, mesh=split, in_specs=in_specs, out_specs=out_specs, check_vma=False
    )
```

```python
import jax
import jax.numpy as jnp
from jax import lax
from jax.experimental import pallas as pl
from jax.experimental.pallas import tpu as pltpu
from jax.sharding import Mesh
from jax.sharding import PartitionSpec as P


BLK = ("blk_0", "blk_1")
BLK_REP = ("blk_0", "blk_1", "rep")

BS = 128
CHUNK = 8
SUBLANES = 8
STEP = 8
PIECE = 4
AHEAD = 3
F32 = jnp.float32
BF16 = jnp.bfloat16
F16 = jnp.float16
VMEM = pltpu.VMEM
SMEM = pltpu.SMEM


def whole(space=VMEM):
    return pl.BlockSpec(memory_space=space)


def near(array):
    return pltpu.with_memory_space_constraint(array, VMEM)


def select_kernel(names, place, table, out):
    reps, named = names.shape
    for peer in range(reps):
        back = jnp.bitwise_xor(place[0], peer)
        for t in range(named):
            out[peer, t] = table[names[back, t]]


def gram_kernel(rows, gram):
    reps, per_owner, width, _ = rows.shape
    total = jnp.zeros(gram.shape, F32)
    for t in range(per_owner):
        total = total + lax.dot_general(
            rows[0, t],
            rows[:, t].reshape(reps * width, BS),
            (((1,), (1,)), ((), ())),
            preferred_element_type=F32,
        )
    gram[...] = total


def fit_kernel(gram, rows, fitted):
    reps, per_owner, width, _ = rows.shape
    rest = gram[...] * gram[...]
    pieces = []
    for _ in range(3):
        piece = rest.astype(BF16)
        rest = rest - piece.astype(F32)
        pieces.append(piece)
    for t in range(per_owner):
        block = rows[:, t].reshape(reps * width, BS)
        value = jnp.dot(pieces[2], block, preferred_element_type=F32)
        value = value + jnp.dot(pieces[1], block, preferred_element_type=F32)
        fitted[t] = value + jnp.dot(pieces[0], block, preferred_element_type=F32)


def fetch(source, target, arrived, piece):
    held = PIECE * CHUNK
    per_slot = BS // held
    slot = piece // per_slot
    rows = pl.ds((piece - slot * per_slot) * held, held)
    return pltpu.make_async_copy(source.at[slot, rows], target.at[slot, rows], arrived.at[piece])


def contract_kernel(
    triples, count, x_far, sel, out,
    x, arrived, fac, low, mid, lower_a, middle_a, lower_b, middle_b, y1, y2, y3,
):
    slots = x.shape[0]
    reps, _, width, _ = sel.shape
    rank = reps * width
    per_slot = BS // CHUNK
    chunks = slots * per_slot
    pieces = chunks // PIECE
    for piece in range(min(AHEAD, pieces)):
        fetch(x_far, x, arrived, piece).start()
    for slot in range(slots):
        for side in range(3):
            turned = sel[:, slot * 3 + side].reshape(rank, BS).astype(F32).T
            if side < 2:
                fac[slot, side] = turned
            if side == 2:
                low[slot] = turned.astype(BF16)
            if side == 1:
                mid[slot] = turned.astype(BF16)
    y2[...] = jnp.zeros_like(y2)
    y3[...] = jnp.zeros_like(y3)

    def multiply(chunk, lower_s, middle_s):
        slot = chunk // per_slot
        row0 = pl.multiple_of(lax.rem(chunk, per_slot) * CHUNK, CHUNK)
        blocks = x[slot, pl.ds(row0, CHUNK)]
        lower_s[...] = jnp.dot(
            blocks.reshape(CHUNK * BS, BS), low[slot], preferred_element_type=F32
        ).reshape(CHUNK, BS, rank)
        turned = jnp.concatenate([blocks[a].T for a in range(CHUNK)], axis=0)
        middle_s[...] = jnp.dot(turned, mid[slot], preferred_element_type=F32).reshape(
            CHUNK, BS, rank
        )

    def reduce(chunk, lower_s, middle_s):
        slot = chunk // per_slot
        row0 = pl.multiple_of(lax.rem(chunk, per_slot) * CHUNK, CHUNK)
        for half in range(rank // BS):
            cols = slice(half * BS, (half + 1) * BS)
            upper_rows = fac[slot, 0, pl.ds(row0, CHUNK), cols]
            spread = [
                jnp.broadcast_to(upper_rows[a : a + 1], (SUBLANES, BS)) for a in range(CHUNK)
            ]
            sums = [jnp.zeros((SUBLANES, BS), F32) for _ in range(CHUNK)]
            for b in range(0, BS, SUBLANES):
                rows = slice(b, b + SUBLANES)
                other = fac[slot, 1, rows, cols]
                second = y2[slot, rows, cols]
                third = y3[slot, rows, cols]
                for a in range(CHUNK):
                    value = lower_s[a, rows, cols]
                    sums[a] = sums[a] + value * other
                    second = second + value * spread[a]
                    third = third + middle_s[a, rows, cols] * spread[a]
                y2[slot, rows, cols] = second
                y3[slot, rows, cols] = third
            y1[slot, pl.ds(row0, CHUNK), cols] = jnp.concatenate(
                [jnp.sum(sums[a], axis=0, keepdims=True) for a in range(CHUNK)], axis=0
            )

    fetch(x_far, x, arrived, 0).wait()
    multiply(0, lower_a, middle_a)

    def several(step, carry):
        for n in range(STEP // PIECE):
            piece = step * (STEP // PIECE) + n + 1

            @pl.when(piece + AHEAD - 1 < pieces)
            def _():
                fetch(x_far, x, arrived, piece + AHEAD - 1).start()

            @pl.when(piece < pieces)
            def _():
                fetch(x_far, x, arrived, piece).wait()

        first = step * STEP
        for n in range(STEP):
            here, there = (lower_a, middle_a), (lower_b, middle_b)
            if n % 2:
                here, there = there, here
            multiply(jnp.minimum(first + n + 1, chunks - 1), *there)
            reduce(first + n, *here)
        return carry

    lax.fori_loop(0, chunks // STEP, several, 0)

    scaled = []
    top = jnp.zeros((1, 1), F32)
    for slot in range(slots):
        i, j, k = triples[slot, 0], triples[slot, 1], triples[slot, 2]
        upper_tie = i == j
        lower_tie = j == k
        alive = jnp.where(slot < count[0], 1.0, 0.0)
        base = jnp.where(upper_tie | lower_tie, 1.0, 2.0) * alive
        dropped = jnp.where(upper_tie & lower_tie, 0.0, base)
        for value, weight in ((y1, base), (y2, dropped), (y3, dropped)):
            scaled.append((value, slot, weight))
            top = jnp.maximum(top, top_of(value[slot]) * weight)
    power = power_of(top)
    scale = stretched(jnp.exp2(power), rank)
    for t, (value, slot, weight) in enumerate(scaled):
        out[:, t * width : (t + 1) * width] = (value[slot].T * (scale * weight)).reshape(
            reps, width, BS
        )
    for peer in range(reps):
        out[peer, len(scaled) * width :] = power


def power_of(top):
    power = 14.0 - jnp.ceil(jnp.log2(jnp.maximum(top, 1e-36)))
    return jnp.broadcast_to(jnp.clip(power, -120.0, 120.0), (SUBLANES, BS))


def stretched(row, count):
    return jnp.concatenate([row] * (count // SUBLANES), axis=0)


def top_of(value):
    return jnp.max(jnp.max(jnp.abs(value), axis=0, keepdims=True), axis=1, keepdims=True)


def scatter_kernel(names, place, parts, out, total):
    reps, named = names.shape
    owners = out.shape[0]
    per_owner = total.shape[0] // owners
    width = total.shape[1]
    total[...] = jnp.zeros_like(total)
    for peer in range(reps):
        back = jnp.bitwise_xor(place[0], peer)
        undo = stretched(jnp.exp2(-parts[peer, named * width :]), width)
        for t in range(named):
            at = names[back, t]
            total[at] = total[at] + parts[peer, t * width : (t + 1) * width] * undo
    power = power_of(top_of(jnp.max(jnp.abs(total[...]), axis=0)))
    scale = stretched(jnp.exp2(power), width)
    for owner in range(owners):
        for t in range(per_owner):
            out[owner, t * width : (t + 1) * width] = total[owner * per_owner + t] * scale
        out[owner, per_owner * width :] = power


def swapped(array, axis, bit):
    peers = lax.axis_size(axis)
    return lax.ppermute(array, axis, [(i, i ^ bit) for i in range(peers)])


def from_each(array, axis):
    array = array[None]
    while array.shape[0] < lax.axis_size(axis):
        array = jnp.concatenate([array, swapped(array, axis, array.shape[0])])
    return array


def summed(array, axis, bits):
    for bit in bits:
        array = array + swapped(array, axis, bit)
    return array


def shards(tensor_blocks, triples, slot_count, factor):
    slots = tensor_blocks.shape[0]
    reps = lax.axis_size("rep")
    owners = lax.axis_size(BLK)
    rows, width = factor.shape
    per_owner = rows // BS
    rank = reps * width
    named = 3 * slots
    place = lax.axis_index("rep").astype(jnp.int32).reshape(1)
    own = factor.T.reshape(width, per_owner, BS).swapaxes(0, 1)

    table = lax.all_to_all(
        jnp.broadcast_to(own[None], (owners, *own.shape)), BLK, 0, 0, tiled=True
    ).reshape(owners * per_owner, width, BS)

    listed = jnp.pad(triples.reshape(1, named).astype(BF16), ((0, 15), (0, BS - named)))
    around = from_each(jnp.concatenate([own.reshape(per_owner * width, BS), listed]), "rep")
    names = around[:, per_owner * width, :named].astype(jnp.int32)
    own_rows = around[:, : per_owner * width].reshape(reps, per_owner, width, BS)
    gram = pl.pallas_call(
        gram_kernel,
        out_shape=jax.ShapeDtypeStruct((width, rank), F32),
        in_specs=[whole()],
        out_specs=whole(),
        compiler_params=pltpu.CompilerParams(vmem_limit_bytes=16 << 20),
        name="gram",
    )(own_rows)

    chosen = pl.pallas_call(
        select_kernel,
        out_shape=VMEM((reps, named, width, BS), BF16),
        in_specs=[whole(SMEM), whole(SMEM), whole()],
        out_specs=whole(),
        compiler_params=pltpu.CompilerParams(vmem_limit_bytes=16 << 20),
        name="select",
    )(names, place, near(table))
    chosen = lax.all_to_all(chosen, "rep", 0, 0, tiled=True)

    gram = summed(gram, "blk_0", (4,))
    gram = summed(gram, "blk_0", (2,))
    gram = summed(gram, "blk_0", (1,))

    parts = pl.pallas_call(
        contract_kernel,
        out_shape=VMEM((reps, named * width + SUBLANES, BS), F32),
        in_specs=[whole(SMEM), whole(SMEM), whole(pltpu.HBM), whole()],
        out_specs=whole(),
        scratch_shapes=[
            VMEM((slots, BS, BS, BS), BF16),
            pltpu.SemaphoreType.DMA((slots * BS // (PIECE * CHUNK),)),
            VMEM((slots, 2, BS, rank), F32),
            VMEM((slots, BS, rank), BF16),
            VMEM((slots, BS, rank), BF16),
            VMEM((CHUNK, BS, rank), F32),
            VMEM((CHUNK, BS, rank), F32),
            VMEM((CHUNK, BS, rank), F32),
            VMEM((CHUNK, BS, rank), F32),
            VMEM((slots, BS, rank), F32),
            VMEM((slots, BS, rank), F32),
            VMEM((slots, BS, rank), F32),
        ],
        compiler_params=pltpu.CompilerParams(vmem_limit_bytes=32 << 20),
        name="contract",
    )(
        triples,
        slot_count,
        pltpu.with_memory_space_constraint(tensor_blocks, pltpu.HBM),
        near(chosen),
    )
    parts = lax.all_to_all(parts.astype(F16), "rep", 0, 0, tiled=True)

    gram = summed(gram, "blk_1", (1,))
    gram = summed(gram, "blk_1", (2,))
    fitted = pl.pallas_call(
        fit_kernel,
        out_shape=jax.ShapeDtypeStruct((per_owner, width, BS), F32),
        in_specs=[whole(), whole()],
        out_specs=whole(),
        compiler_params=pltpu.CompilerParams(vmem_limit_bytes=16 << 20),
        name="fit",
    )(gram, own_rows)

    held = per_owner * width
    scaled = pl.pallas_call(
        scatter_kernel,
        out_shape=VMEM((owners, held + SUBLANES, BS), F32),
        in_specs=[whole(SMEM), whole(SMEM), whole()],
        out_specs=whole(),
        scratch_shapes=[VMEM((owners * per_owner, width, BS), F32)],
        compiler_params=pltpu.CompilerParams(vmem_limit_bytes=16 << 20),
        name="scatter",
    )(names, place, near(parts.astype(F32)))
    arrived = lax.all_to_all(scaled.astype(F16), BLK, 0, 0, tiled=True)
    arrived = arrived.astype(F32)
    moment = (arrived[:, :held] * jnp.exp2(-arrived[:, held:, :1][:, :1])).sum(0)
    gradient = fitted - moment.reshape(per_owner, width, BS)
    return gradient.swapaxes(0, 1).reshape(width, rows).T


def solution(mesh):
    split = Mesh(mesh.devices.reshape(8, 4, mesh.shape["rep"]), ("blk_0", "blk_1", "rep"))
    in_specs = (P(BLK_REP, None, None, None), P(BLK_REP, None), P(BLK_REP), P(BLK, "rep"))
    out_specs = P(BLK, "rep")
    return jax.shard_map(
        shards, mesh=split, in_specs=in_specs, out_specs=out_specs, check_vma=False
    )
```

```python
import jax
import jax.numpy as jnp
from jax import lax
from jax.experimental import pallas as pl
from jax.experimental.pallas import tpu as pltpu
from jax.sharding import Mesh
from jax.sharding import PartitionSpec as P


BLK = ("blk_0", "blk_1")
BLK_REP = ("blk_0", "blk_1", "rep")

BS = 128
CHUNK = 8
SUBLANES = 8
STEP = 8
PIECE = 4
GROUP = 2
AHEAD = 3
F32 = jnp.float32
BF16 = jnp.bfloat16
F16 = jnp.float16
VMEM = pltpu.VMEM
SMEM = pltpu.SMEM


def whole(space=VMEM):
    return pl.BlockSpec(memory_space=space)


def near(array):
    return pltpu.with_memory_space_constraint(array, VMEM)


def select_kernel(names, place, table, out):
    reps, named = names.shape
    for peer in range(reps):
        back = jnp.bitwise_xor(place[0], peer)
        for t in range(named):
            out[peer, t] = table[names[back, t]]


def gram_kernel(rows, gram):
    reps, per_owner, width, _ = rows.shape
    total = jnp.zeros(gram.shape, F32)
    for t in range(per_owner):
        total = total + lax.dot_general(
            rows[0, t],
            rows[:, t].reshape(reps * width, BS),
            (((1,), (1,)), ((), ())),
            preferred_element_type=F32,
        )
    gram[...] = total


def fit_kernel(gram, rows, fitted):
    reps, per_owner, width, _ = rows.shape
    rest = gram[...] * gram[...]
    pieces = []
    for _ in range(3):
        piece = rest.astype(BF16)
        rest = rest - piece.astype(F32)
        pieces.append(piece)
    for t in range(per_owner):
        block = rows[:, t].reshape(reps * width, BS)
        value = jnp.dot(pieces[2], block, preferred_element_type=F32)
        value = value + jnp.dot(pieces[1], block, preferred_element_type=F32)
        fitted[t] = value + jnp.dot(pieces[0], block, preferred_element_type=F32)


def fetch(source, target, arrived, piece):
    held = PIECE * CHUNK
    per_slot = BS // held
    slot = piece // per_slot
    rows = pl.ds((piece - slot * per_slot) * held, held)
    return pltpu.make_async_copy(source.at[slot, rows], target.at[slot, rows], arrived.at[piece])


def contract_kernel(
    triples, count, x_far, sel, out,
    x, arrived, fac, low, mid, y1, y2, y3,
):
    slots = x.shape[0]
    reps, _, width, _ = sel.shape
    rank = reps * width
    per_slot = BS // CHUNK
    chunks = slots * per_slot
    pieces = chunks // PIECE
    for piece in range(min(AHEAD, pieces)):
        fetch(x_far, x, arrived, piece).start()
    for slot in range(slots):
        for side in range(3):
            turned = sel[:, slot * 3 + side].reshape(rank, BS).astype(F32).T
            if side < 2:
                fac[slot, side] = turned
            if side == 2:
                low[slot] = turned.astype(BF16)
            if side == 1:
                mid[slot] = turned.astype(BF16)
    y2[...] = jnp.zeros_like(y2)
    y3[...] = jnp.zeros_like(y3)

    def several(step, carry):
        for n in range(STEP // PIECE):
            piece = step * (STEP // PIECE) + n

            @pl.when(piece + AHEAD < pieces)
            def _():
                fetch(x_far, x, arrived, piece + AHEAD).start()

            fetch(x_far, x, arrived, piece).wait()
        for n in range(STEP):
            chunk = step * STEP + n
            slot = chunk // per_slot
            row0 = pl.multiple_of(lax.rem(chunk, per_slot) * CHUNK, CHUNK)
            lower = low[slot]
            middle = mid[slot]
            firsts = [[] for _ in range(rank // BS)]
            for a0 in range(0, CHUNK, GROUP):
                blocks = x[slot, pl.ds(row0 + a0, GROUP)]
                ls = jnp.dot(
                    blocks.reshape(GROUP * BS, BS), lower, preferred_element_type=F32
                ).reshape(GROUP, BS, rank)
                turned = jnp.concatenate([blocks[a].T for a in range(GROUP)], axis=0)
                ms = jnp.dot(turned, middle, preferred_element_type=F32).reshape(GROUP, BS, rank)
                upper = fac[slot, 0, pl.ds(row0, CHUNK)]
                for half in range(rank // BS):
                    cols = slice(half * BS, (half + 1) * BS)
                    spread = [
                        jnp.broadcast_to(upper[a0 + a : a0 + a + 1, cols], (SUBLANES, BS))
                        for a in range(GROUP)
                    ]
                    sums = [jnp.zeros((SUBLANES, BS), F32) for _ in range(GROUP)]
                    for b in range(0, BS, SUBLANES):
                        rows = slice(b, b + SUBLANES)
                        other = fac[slot, 1, rows, cols]
                        second = y2[slot, rows, cols]
                        third = y3[slot, rows, cols]
                        for a in range(GROUP):
                            value = ls[a, rows, cols]
                            sums[a] = sums[a] + value * other
                            second = second + value * spread[a]
                            third = third + ms[a, rows, cols] * spread[a]
                        y2[slot, rows, cols] = second
                        y3[slot, rows, cols] = third
                    firsts[half].extend(jnp.sum(v, axis=0, keepdims=True) for v in sums)
            for half in range(rank // BS):
                cols = slice(half * BS, (half + 1) * BS)
                y1[slot, pl.ds(row0, CHUNK), cols] = jnp.concatenate(firsts[half], axis=0)
        return carry

    lax.fori_loop(0, chunks // STEP, several, 0)

    scaled = []
    top = jnp.zeros((1, 1), F32)
    for slot in range(slots):
        i, j, k = triples[slot, 0], triples[slot, 1], triples[slot, 2]
        upper_tie = i == j
        lower_tie = j == k
        alive = jnp.where(slot < count[0], 1.0, 0.0)
        base = jnp.where(upper_tie | lower_tie, 1.0, 2.0) * alive
        dropped = jnp.where(upper_tie & lower_tie, 0.0, base)
        for value, weight in ((y1, base), (y2, dropped), (y3, dropped)):
            scaled.append((value, slot, weight))
            top = jnp.maximum(top, top_of(value[slot]) * weight)
    power = power_of(top)
    scale = stretched(jnp.exp2(power), rank)
    for t, (value, slot, weight) in enumerate(scaled):
        out[:, t * width : (t + 1) * width] = (value[slot].T * (scale * weight)).reshape(
            reps, width, BS
        )
    for peer in range(reps):
        out[peer, len(scaled) * width :] = power


def power_of(top):
    power = 14.0 - jnp.ceil(jnp.log2(jnp.maximum(top, 1e-36)))
    return jnp.broadcast_to(jnp.clip(power, -120.0, 120.0), (SUBLANES, BS))


def stretched(row, count):
    return jnp.concatenate([row] * (count // SUBLANES), axis=0)


def top_of(value):
    return jnp.max(jnp.max(jnp.abs(value), axis=0, keepdims=True), axis=1, keepdims=True)


def scatter_kernel(names, place, parts, out, total):
    reps, named = names.shape
    owners = out.shape[0]
    per_owner = total.shape[0] // owners
    width = total.shape[1]
    total[...] = jnp.zeros_like(total)
    for peer in range(reps):
        back = jnp.bitwise_xor(place[0], peer)
        undo = stretched(jnp.exp2(-parts[peer, named * width :]), width)
        for t in range(named):
            at = names[back, t]
            total[at] = total[at] + parts[peer, t * width : (t + 1) * width] * undo
    power = power_of(top_of(jnp.max(jnp.abs(total[...]), axis=0)))
    scale = stretched(jnp.exp2(power), width)
    for owner in range(owners):
        for t in range(per_owner):
            out[owner, t * width : (t + 1) * width] = total[owner * per_owner + t] * scale
        out[owner, per_owner * width :] = power


def swapped(array, axis, bit):
    peers = lax.axis_size(axis)
    return lax.ppermute(array, axis, [(i, i ^ bit) for i in range(peers)])


def from_each(array, axis):
    array = array[None]
    while array.shape[0] < lax.axis_size(axis):
        array = jnp.concatenate([array, swapped(array, axis, array.shape[0])])
    return array


def summed(array, axis, bits):
    for bit in bits:
        array = array + swapped(array, axis, bit)
    return array


def shards(tensor_blocks, triples, slot_count, factor):
    slots = tensor_blocks.shape[0]
    reps = lax.axis_size("rep")
    owners = lax.axis_size(BLK)
    rows, width = factor.shape
    per_owner = rows // BS
    rank = reps * width
    named = 3 * slots
    place = lax.axis_index("rep").astype(jnp.int32).reshape(1)
    own = factor.T.reshape(width, per_owner, BS).swapaxes(0, 1)

    table = lax.all_to_all(
        jnp.broadcast_to(own[None], (owners, *own.shape)), BLK, 0, 0, tiled=True
    ).reshape(owners * per_owner, width, BS)

    listed = jnp.pad(triples.reshape(1, named).astype(BF16), ((0, 15), (0, BS - named)))
    around = from_each(jnp.concatenate([own.reshape(per_owner * width, BS), listed]), "rep")
    names = around[:, per_owner * width, :named].astype(jnp.int32)
    own_rows = around[:, : per_owner * width].reshape(reps, per_owner, width, BS)
    gram = pl.pallas_call(
        gram_kernel,
        out_shape=jax.ShapeDtypeStruct((width, rank), F32),
        in_specs=[whole()],
        out_specs=whole(),
        compiler_params=pltpu.CompilerParams(vmem_limit_bytes=16 << 20),
        name="gram",
    )(own_rows)

    chosen = pl.pallas_call(
        select_kernel,
        out_shape=VMEM((reps, named, width, BS), BF16),
        in_specs=[whole(SMEM), whole(SMEM), whole()],
        out_specs=whole(),
        compiler_params=pltpu.CompilerParams(vmem_limit_bytes=16 << 20),
        name="select",
    )(names, place, near(table))
    chosen = lax.all_to_all(chosen, "rep", 0, 0, tiled=True)

    gram = summed(gram, "blk_0", (4,))
    gram = summed(gram, "blk_0", (2,))
    gram = summed(gram, "blk_0", (1,))

    parts = pl.pallas_call(
        contract_kernel,
        out_shape=VMEM((reps, named * width + SUBLANES, BS), F32),
        in_specs=[whole(SMEM), whole(SMEM), whole(pltpu.HBM), whole()],
        out_specs=whole(),
        scratch_shapes=[
            VMEM((slots, BS, BS, BS), BF16),
            pltpu.SemaphoreType.DMA((slots * BS // (PIECE * CHUNK),)),
            VMEM((slots, 2, BS, rank), F32),
            VMEM((slots, BS, rank), BF16),
            VMEM((slots, BS, rank), BF16),
            VMEM((slots, BS, rank), F32),
            VMEM((slots, BS, rank), F32),
            VMEM((slots, BS, rank), F32),
        ],
        compiler_params=pltpu.CompilerParams(vmem_limit_bytes=32 << 20),
        name="contract",
    )(
        triples,
        slot_count,
        pltpu.with_memory_space_constraint(tensor_blocks, pltpu.HBM),
        near(chosen),
    )
    parts = lax.all_to_all(parts.astype(F16), "rep", 0, 0, tiled=True)

    gram = summed(gram, "blk_1", (1,))
    gram = summed(gram, "blk_1", (2,))
    fitted = pl.pallas_call(
        fit_kernel,
        out_shape=jax.ShapeDtypeStruct((per_owner, width, BS), F32),
        in_specs=[whole(), whole()],
        out_specs=whole(),
        compiler_params=pltpu.CompilerParams(vmem_limit_bytes=16 << 20),
        name="fit",
    )(gram, own_rows)

    held = per_owner * width
    scaled = pl.pallas_call(
        scatter_kernel,
        out_shape=VMEM((owners, held + SUBLANES, BS), F32),
        in_specs=[whole(SMEM), whole(SMEM), whole()],
        out_specs=whole(),
        scratch_shapes=[VMEM((owners * per_owner, width, BS), F32)],
        compiler_params=pltpu.CompilerParams(vmem_limit_bytes=16 << 20),
        name="scatter",
    )(names, place, near(parts.astype(F32)))
    arrived = lax.all_to_all(scaled.astype(F16), BLK, 0, 0, tiled=True)
    arrived = arrived.astype(F32)
    moment = (arrived[:, :held] * jnp.exp2(-arrived[:, held:, :1][:, :1])).sum(0)
    gradient = fitted - moment.reshape(per_owner, width, BS)
    return gradient.swapaxes(0, 1).reshape(width, rows).T


def solution(mesh):
    split = Mesh(mesh.devices.reshape(8, 4, mesh.shape["rep"]), ("blk_0", "blk_1", "rep"))
    in_specs = (P(BLK_REP, None, None, None), P(BLK_REP, None), P(BLK_REP), P(BLK, "rep"))
    out_specs = P(BLK, "rep")
    return jax.shard_map(
        shards, mesh=split, in_specs=in_specs, out_specs=out_specs, check_vma=False
    )
```

```python
import jax
import jax.numpy as jnp
from jax import lax
from jax.experimental import pallas as pl
from jax.experimental.pallas import tpu as pltpu
from jax.sharding import Mesh
from jax.sharding import PartitionSpec as P


BLK = ("blk_0", "blk_1")
BLK_REP = ("blk_0", "blk_1", "rep")

BS = 128
CHUNK = 8
SUBLANES = 8
STEP = 8
PIECE = 4
GROUP = 2
AHEAD = 3
F32 = jnp.float32
BF16 = jnp.bfloat16
F16 = jnp.float16
VMEM = pltpu.VMEM
SMEM = pltpu.SMEM


def whole(space=VMEM):
    return pl.BlockSpec(memory_space=space)


def near(array):
    return pltpu.with_memory_space_constraint(array, VMEM)


def select_kernel(names, place, table, out):
    reps, named = names.shape
    for peer in range(reps):
        back = jnp.bitwise_xor(place[0], peer)
        for t in range(named):
            out[peer, t] = table[names[back, t]]


def gram_kernel(rows, gram):
    reps, per_owner, width, _ = rows.shape
    total = jnp.zeros(gram.shape, F32)
    for t in range(per_owner):
        total = total + lax.dot_general(
            rows[0, t],
            rows[:, t].reshape(reps * width, BS),
            (((1,), (1,)), ((), ())),
            preferred_element_type=F32,
        )
    gram[...] = total


def fit_kernel(gram, rows, fitted):
    reps, per_owner, width, _ = rows.shape
    rest = gram[...] * gram[...]
    pieces = []
    for _ in range(3):
        piece = rest.astype(BF16)
        rest = rest - piece.astype(F32)
        pieces.append(piece)
    for t in range(per_owner):
        block = rows[:, t].reshape(reps * width, BS)
        value = jnp.dot(pieces[2], block, preferred_element_type=F32)
        value = value + jnp.dot(pieces[1], block, preferred_element_type=F32)
        fitted[t] = value + jnp.dot(pieces[0], block, preferred_element_type=F32)


def fetch(source, target, arrived, piece):
    held = PIECE * CHUNK
    per_slot = BS // held
    slot = piece // per_slot
    rows = pl.ds((piece - slot * per_slot) * held, held)
    return pltpu.make_async_copy(source.at[slot, rows], target.at[slot, rows], arrived.at[piece])


def contract_kernel(
    triples, count, head, x_far, sel, out,
    x, arrived, fac, low, mid, y1, y2, y3,
):
    slots = x.shape[0]
    reps, _, width, _ = sel.shape
    rank = reps * width
    per_slot = BS // CHUNK
    chunks = slots * per_slot
    pieces = chunks // PIECE
    skipped = STEP // PIECE
    for piece in range(skipped, skipped + AHEAD):
        fetch(x_far, x, arrived, piece).start()
    for slot in range(slots):
        for side in range(3):
            turned = sel[:, slot * 3 + side].reshape(rank, BS).astype(F32).T
            if side < 2:
                fac[slot, side] = turned
            if side == 2:
                low[slot] = turned.astype(BF16)
            if side == 1:
                mid[slot] = turned.astype(BF16)
    y2[...] = jnp.zeros_like(y2)
    y3[...] = jnp.zeros_like(y3)

    def several(step, source):
        for n in range(STEP):
            chunk = step * STEP + n
            slot = chunk // per_slot
            row0 = (chunk - slot * per_slot) * CHUNK
            if not isinstance(row0, int):
                row0 = pl.multiple_of(row0, CHUNK)
            lower = low[slot]
            middle = mid[slot]
            firsts = [[] for _ in range(rank // BS)]
            for a0 in range(0, CHUNK, GROUP):
                blocks = source(slot, pl.ds(row0 + a0, GROUP))
                ls = jnp.dot(
                    blocks.reshape(GROUP * BS, BS), lower, preferred_element_type=F32
                ).reshape(GROUP, BS, rank)
                turned = jnp.concatenate([blocks[a].T for a in range(GROUP)], axis=0)
                ms = jnp.dot(turned, middle, preferred_element_type=F32).reshape(GROUP, BS, rank)
                upper = fac[slot, 0, pl.ds(row0, CHUNK)]
                for half in range(rank // BS):
                    cols = slice(half * BS, (half + 1) * BS)
                    spread = [
                        jnp.broadcast_to(upper[a0 + a : a0 + a + 1, cols], (SUBLANES, BS))
                        for a in range(GROUP)
                    ]
                    sums = [jnp.zeros((SUBLANES, BS), F32) for _ in range(GROUP)]
                    for b in range(0, BS, SUBLANES):
                        rows = slice(b, b + SUBLANES)
                        other = fac[slot, 1, rows, cols]
                        second = y2[slot, rows, cols]
                        third = y3[slot, rows, cols]
                        for a in range(GROUP):
                            value = ls[a, rows, cols]
                            sums[a] = sums[a] + value * other
                            second = second + value * spread[a]
                            third = third + ms[a, rows, cols] * spread[a]
                        y2[slot, rows, cols] = second
                        y3[slot, rows, cols] = third
                    firsts[half].extend(jnp.sum(v, axis=0, keepdims=True) for v in sums)
            for half in range(rank // BS):
                cols = slice(half * BS, (half + 1) * BS)
                y1[slot, pl.ds(row0, CHUNK), cols] = jnp.concatenate(firsts[half], axis=0)

    several(0, lambda slot, rows: head[rows])

    def later(step, carry):
        for n in range(STEP // PIECE):
            piece = step * (STEP // PIECE) + n

            @pl.when(piece + AHEAD < pieces)
            def _():
                fetch(x_far, x, arrived, piece + AHEAD).start()

            fetch(x_far, x, arrived, piece).wait()
        several(step, lambda slot, rows: x[slot, rows])
        return carry

    lax.fori_loop(1, chunks // STEP, later, 0)

    scaled = []
    top = jnp.zeros((1, 1), F32)
    for slot in range(slots):
        i, j, k = triples[slot, 0], triples[slot, 1], triples[slot, 2]
        upper_tie = i == j
        lower_tie = j == k
        alive = jnp.where(slot < count[0], 1.0, 0.0)
        base = jnp.where(upper_tie | lower_tie, 1.0, 2.0) * alive
        dropped = jnp.where(upper_tie & lower_tie, 0.0, base)
        for value, weight in ((y1, base), (y2, dropped), (y3, dropped)):
            scaled.append((value, slot, weight))
            top = jnp.maximum(top, top_of(value[slot]) * weight)
    power = power_of(top)
    scale = stretched(jnp.exp2(power), rank)
    for t, (value, slot, weight) in enumerate(scaled):
        out[:, t * width : (t + 1) * width] = (value[slot].T * (scale * weight)).reshape(
            reps, width, BS
        )
    for peer in range(reps):
        out[peer, len(scaled) * width :] = power


def power_of(top):
    power = 14.0 - jnp.ceil(jnp.log2(jnp.maximum(top, 1e-36)))
    return jnp.broadcast_to(jnp.clip(power, -120.0, 120.0), (SUBLANES, BS))


def stretched(row, count):
    return jnp.concatenate([row] * (count // SUBLANES), axis=0)


def top_of(value):
    return jnp.max(jnp.max(jnp.abs(value), axis=0, keepdims=True), axis=1, keepdims=True)


def scatter_kernel(names, place, parts, out, total):
    reps, named = names.shape
    owners = out.shape[0]
    per_owner = total.shape[0] // owners
    width = total.shape[1]
    total[...] = jnp.zeros_like(total)
    for peer in range(reps):
        back = jnp.bitwise_xor(place[0], peer)
        undo = stretched(jnp.exp2(-parts[peer, named * width :]), width)
        for t in range(named):
            at = names[back, t]
            total[at] = total[at] + parts[peer, t * width : (t + 1) * width] * undo
    power = power_of(top_of(jnp.max(jnp.abs(total[...]), axis=0)))
    scale = stretched(jnp.exp2(power), width)
    for owner in range(owners):
        for t in range(per_owner):
            out[owner, t * width : (t + 1) * width] = total[owner * per_owner + t] * scale
        out[owner, per_owner * width :] = power


def swapped(array, axis, bit):
    peers = lax.axis_size(axis)
    return lax.ppermute(array, axis, [(i, i ^ bit) for i in range(peers)])


def from_each(array, axis):
    array = array[None]
    while array.shape[0] < lax.axis_size(axis):
        array = jnp.concatenate([array, swapped(array, axis, array.shape[0])])
    return array


def summed(array, axis, bits):
    for bit in bits:
        array = array + swapped(array, axis, bit)
    return array


def shards(tensor_blocks, triples, slot_count, factor):
    slots = tensor_blocks.shape[0]
    reps = lax.axis_size("rep")
    owners = lax.axis_size(BLK)
    rows, width = factor.shape
    per_owner = rows // BS
    rank = reps * width
    named = 3 * slots
    place = lax.axis_index("rep").astype(jnp.int32).reshape(1)
    own = factor.T.reshape(width, per_owner, BS).swapaxes(0, 1)

    table = lax.all_to_all(
        jnp.broadcast_to(own[None], (owners, *own.shape)), BLK, 0, 0, tiled=True
    ).reshape(owners * per_owner, width, BS)

    listed = jnp.pad(triples.reshape(1, named).astype(BF16), ((0, 15), (0, BS - named)))
    around = from_each(jnp.concatenate([own.reshape(per_owner * width, BS), listed]), "rep")
    names = around[:, per_owner * width, :named].astype(jnp.int32)
    own_rows = around[:, : per_owner * width].reshape(reps, per_owner, width, BS)
    gram = pl.pallas_call(
        gram_kernel,
        out_shape=jax.ShapeDtypeStruct((width, rank), F32),
        in_specs=[whole()],
        out_specs=whole(),
        compiler_params=pltpu.CompilerParams(vmem_limit_bytes=16 << 20),
        name="gram",
    )(own_rows)

    chosen = pl.pallas_call(
        select_kernel,
        out_shape=VMEM((reps, named, width, BS), BF16),
        in_specs=[whole(SMEM), whole(SMEM), whole()],
        out_specs=whole(),
        compiler_params=pltpu.CompilerParams(vmem_limit_bytes=16 << 20),
        name="select",
    )(names, place, near(table))
    chosen = lax.all_to_all(chosen, "rep", 0, 0, tiled=True)

    gram = summed(gram, "blk_0", (4,))
    gram = summed(gram, "blk_0", (2,))
    gram = summed(gram, "blk_0", (1,))

    head = tensor_blocks[0, : STEP * CHUNK]
    parts = pl.pallas_call(
        contract_kernel,
        out_shape=VMEM((reps, named * width + SUBLANES, BS), F32),
        in_specs=[whole(SMEM), whole(SMEM), whole(), whole(pltpu.HBM), whole()],
        out_specs=whole(),
        scratch_shapes=[
            VMEM((slots, BS, BS, BS), BF16),
            pltpu.SemaphoreType.DMA((slots * BS // (PIECE * CHUNK),)),
            VMEM((slots, 2, BS, rank), F32),
            VMEM((slots, BS, rank), BF16),
            VMEM((slots, BS, rank), BF16),
            VMEM((slots, BS, rank), F32),
            VMEM((slots, BS, rank), F32),
            VMEM((slots, BS, rank), F32),
        ],
        compiler_params=pltpu.CompilerParams(vmem_limit_bytes=32 << 20),
        name="contract",
    )(
        triples,
        slot_count,
        near(head),
        pltpu.with_memory_space_constraint(tensor_blocks, pltpu.HBM),
        near(chosen),
    )
    parts = lax.all_to_all(parts.astype(F16), "rep", 0, 0, tiled=True)

    gram = summed(gram, "blk_1", (1,))
    gram = summed(gram, "blk_1", (2,))
    fitted = pl.pallas_call(
        fit_kernel,
        out_shape=jax.ShapeDtypeStruct((per_owner, width, BS), F32),
        in_specs=[whole(), whole()],
        out_specs=whole(),
        compiler_params=pltpu.CompilerParams(vmem_limit_bytes=16 << 20),
        name="fit",
    )(gram, own_rows)

    held = per_owner * width
    scaled = pl.pallas_call(
        scatter_kernel,
        out_shape=VMEM((owners, held + SUBLANES, BS), F32),
        in_specs=[whole(SMEM), whole(SMEM), whole()],
        out_specs=whole(),
        scratch_shapes=[VMEM((owners * per_owner, width, BS), F32)],
        compiler_params=pltpu.CompilerParams(vmem_limit_bytes=16 << 20),
        name="scatter",
    )(names, place, near(parts.astype(F32)))
    arrived = lax.all_to_all(scaled.astype(F16), BLK, 0, 0, tiled=True)
    arrived = arrived.astype(F32)
    moment = (arrived[:, :held] * jnp.exp2(-arrived[:, held:, :1][:, :1])).sum(0)
    gradient = fitted - moment.reshape(per_owner, width, BS)
    return gradient.swapaxes(0, 1).reshape(width, rows).T


def solution(mesh):
    split = Mesh(mesh.devices.reshape(8, 4, mesh.shape["rep"]), ("blk_0", "blk_1", "rep"))
    in_specs = (P(BLK_REP, None, None, None), P(BLK_REP, None), P(BLK_REP), P(BLK, "rep"))
    out_specs = P(BLK, "rep")
    return jax.shard_map(
        shards, mesh=split, in_specs=in_specs, out_specs=out_specs, check_vma=False
    )
```

```python
import jax
import jax.numpy as jnp
from jax import lax
from jax.experimental import pallas as pl
from jax.experimental.pallas import tpu as pltpu
from jax.sharding import Mesh
from jax.sharding import PartitionSpec as P


BLK = ("blk_0", "blk_1")
BLK_REP = ("blk_0", "blk_1", "rep")

BS = 128
CHUNK = 8
SUBLANES = 8
STEP = 8
PIECE = 4
GROUP = 2
AHEAD = 3
F32 = jnp.float32
BF16 = jnp.bfloat16
F16 = jnp.float16
VMEM = pltpu.VMEM
SMEM = pltpu.SMEM


def whole(space=VMEM):
    return pl.BlockSpec(memory_space=space)


def near(array):
    return pltpu.with_memory_space_constraint(array, VMEM)


def select_kernel(names, place, table, out):
    reps, named = names.shape
    for peer in range(reps):
        back = jnp.bitwise_xor(place[0], peer)
        for t in range(named):
            out[peer, t] = table[names[back, t]]


def gram_kernel(rows, gram):
    reps, per_owner, width, _ = rows.shape
    total = jnp.zeros(gram.shape, F32)
    for t in range(per_owner):
        total = total + lax.dot_general(
            rows[0, t],
            rows[:, t].reshape(reps * width, BS),
            (((1,), (1,)), ((), ())),
            preferred_element_type=F32,
        )
    gram[...] = total


def fit_kernel(gram, rows, fitted):
    reps, per_owner, width, _ = rows.shape
    rest = gram[...] * gram[...]
    pieces = []
    for _ in range(3):
        piece = rest.astype(BF16)
        rest = rest - piece.astype(F32)
        pieces.append(piece)
    for t in range(per_owner):
        block = rows[:, t].reshape(reps * width, BS)
        value = jnp.dot(pieces[2], block, preferred_element_type=F32)
        value = value + jnp.dot(pieces[1], block, preferred_element_type=F32)
        fitted[t] = value + jnp.dot(pieces[0], block, preferred_element_type=F32)


def fetch(source, target, arrived, piece):
    held = PIECE * CHUNK
    per_slot = BS // held
    slot = piece // per_slot
    rows = pl.ds((piece - slot * per_slot) * held, held)
    return pltpu.make_async_copy(source.at[slot, rows], target.at[slot, rows], arrived.at[piece])


def contract_kernel(
    triples, count, head, x_far, sel, out,
    x, arrived, fac, low, mid, y1, y2, y3,
):
    slots = x.shape[0]
    reps, _, width, _ = sel.shape
    rank = reps * width
    per_slot = BS // CHUNK
    chunks = slots * per_slot
    pieces = chunks // PIECE
    skipped = STEP // PIECE
    for piece in range(skipped, skipped + AHEAD):
        fetch(x_far, x, arrived, piece).start()

    def placed(n, carry):
        rows = pl.ds(pl.multiple_of(n * CHUNK, CHUNK), CHUNK)
        x[0, rows] = head[rows]
        return carry

    lax.fori_loop(0, STEP, placed, 0)
    for slot in range(slots):
        for side in range(3):
            turned = sel[:, slot * 3 + side].reshape(rank, BS).astype(F32).T
            if side < 2:
                fac[slot, side] = turned
            if side == 2:
                low[slot] = turned.astype(BF16)
            if side == 1:
                mid[slot] = turned.astype(BF16)
    y2[...] = jnp.zeros_like(y2)
    y3[...] = jnp.zeros_like(y3)

    def several(step, carry):
        for n in range(STEP // PIECE):
            piece = step * (STEP // PIECE) + n

            @pl.when((step > 0) & (piece + AHEAD < pieces))
            def _():
                fetch(x_far, x, arrived, piece + AHEAD).start()

            @pl.when(step > 0)
            def _():
                fetch(x_far, x, arrived, piece).wait()

        for n in range(STEP):
            chunk = step * STEP + n
            slot = chunk // per_slot
            row0 = pl.multiple_of(lax.rem(chunk, per_slot) * CHUNK, CHUNK)
            lower = low[slot]
            middle = mid[slot]
            firsts = [[] for _ in range(rank // BS)]
            for a0 in range(0, CHUNK, GROUP):
                blocks = x[slot, pl.ds(row0 + a0, GROUP)]
                ls = jnp.dot(
                    blocks.reshape(GROUP * BS, BS), lower, preferred_element_type=F32
                ).reshape(GROUP, BS, rank)
                turned = jnp.concatenate([blocks[a].T for a in range(GROUP)], axis=0)
                ms = jnp.dot(turned, middle, preferred_element_type=F32).reshape(GROUP, BS, rank)
                upper = fac[slot, 0, pl.ds(row0, CHUNK)]
                for half in range(rank // BS):
                    cols = slice(half * BS, (half + 1) * BS)
                    spread = [
                        jnp.broadcast_to(upper[a0 + a : a0 + a + 1, cols], (SUBLANES, BS))
                        for a in range(GROUP)
                    ]
                    sums = [jnp.zeros((SUBLANES, BS), F32) for _ in range(GROUP)]
                    for b in range(0, BS, SUBLANES):
                        rows = slice(b, b + SUBLANES)
                        other = fac[slot, 1, rows, cols]
                        second = y2[slot, rows, cols]
                        third = y3[slot, rows, cols]
                        for a in range(GROUP):
                            value = ls[a, rows, cols]
                            sums[a] = sums[a] + value * other
                            second = second + value * spread[a]
                            third = third + ms[a, rows, cols] * spread[a]
                        y2[slot, rows, cols] = second
                        y3[slot, rows, cols] = third
                    firsts[half].extend(jnp.sum(v, axis=0, keepdims=True) for v in sums)
            for half in range(rank // BS):
                cols = slice(half * BS, (half + 1) * BS)
                y1[slot, pl.ds(row0, CHUNK), cols] = jnp.concatenate(firsts[half], axis=0)
        return carry

    lax.fori_loop(0, chunks // STEP, several, 0)

    scaled = []
    top = jnp.zeros((1, 1), F32)
    for slot in range(slots):
        i, j, k = triples[slot, 0], triples[slot, 1], triples[slot, 2]
        upper_tie = i == j
        lower_tie = j == k
        alive = jnp.where(slot < count[0], 1.0, 0.0)
        base = jnp.where(upper_tie | lower_tie, 1.0, 2.0) * alive
        dropped = jnp.where(upper_tie & lower_tie, 0.0, base)
        for value, weight in ((y1, base), (y2, dropped), (y3, dropped)):
            scaled.append((value, slot, weight))
            top = jnp.maximum(top, top_of(value[slot]) * weight)
    power = power_of(top)
    scale = stretched(jnp.exp2(power), rank)
    for t, (value, slot, weight) in enumerate(scaled):
        out[:, t * width : (t + 1) * width] = (value[slot].T * (scale * weight)).reshape(
            reps, width, BS
        )
    for peer in range(reps):
        out[peer, len(scaled) * width :] = power


def power_of(top):
    power = 14.0 - jnp.ceil(jnp.log2(jnp.maximum(top, 1e-36)))
    return jnp.broadcast_to(jnp.clip(power, -120.0, 120.0), (SUBLANES, BS))


def stretched(row, count):
    return jnp.concatenate([row] * (count // SUBLANES), axis=0)


def top_of(value):
    return jnp.max(jnp.max(jnp.abs(value), axis=0, keepdims=True), axis=1, keepdims=True)


def scatter_kernel(names, place, parts, out, total):
    reps, named = names.shape
    owners = out.shape[0]
    per_owner = total.shape[0] // owners
    width = total.shape[1]
    total[...] = jnp.zeros_like(total)
    for peer in range(reps):
        back = jnp.bitwise_xor(place[0], peer)
        undo = stretched(jnp.exp2(-parts[peer, named * width :]), width)
        for t in range(named):
            at = names[back, t]
            total[at] = total[at] + parts[peer, t * width : (t + 1) * width] * undo
    power = power_of(top_of(jnp.max(jnp.abs(total[...]), axis=0)))
    scale = stretched(jnp.exp2(power), width)
    for owner in range(owners):
        for t in range(per_owner):
            out[owner, t * width : (t + 1) * width] = total[owner * per_owner + t] * scale
        out[owner, per_owner * width :] = power


def swapped(array, axis, bit):
    peers = lax.axis_size(axis)
    return lax.ppermute(array, axis, [(i, i ^ bit) for i in range(peers)])


def from_each(array, axis):
    array = array[None]
    while array.shape[0] < lax.axis_size(axis):
        array = jnp.concatenate([array, swapped(array, axis, array.shape[0])])
    return array


def summed(array, axis, bits):
    for bit in bits:
        array = array + swapped(array, axis, bit)
    return array


def shards(tensor_blocks, triples, slot_count, factor):
    slots = tensor_blocks.shape[0]
    reps = lax.axis_size("rep")
    owners = lax.axis_size(BLK)
    rows, width = factor.shape
    per_owner = rows // BS
    rank = reps * width
    named = 3 * slots
    place = lax.axis_index("rep").astype(jnp.int32).reshape(1)
    own = factor.T.reshape(width, per_owner, BS).swapaxes(0, 1)

    table = lax.all_to_all(
        jnp.broadcast_to(own[None], (owners, *own.shape)), BLK, 0, 0, tiled=True
    ).reshape(owners * per_owner, width, BS)

    listed = jnp.pad(triples.reshape(1, named).astype(BF16), ((0, 15), (0, BS - named)))
    around = from_each(jnp.concatenate([own.reshape(per_owner * width, BS), listed]), "rep")
    names = around[:, per_owner * width, :named].astype(jnp.int32)
    own_rows = around[:, : per_owner * width].reshape(reps, per_owner, width, BS)
    gram = pl.pallas_call(
        gram_kernel,
        out_shape=jax.ShapeDtypeStruct((width, rank), F32),
        in_specs=[whole()],
        out_specs=whole(),
        compiler_params=pltpu.CompilerParams(vmem_limit_bytes=16 << 20),
        name="gram",
    )(own_rows)

    chosen = pl.pallas_call(
        select_kernel,
        out_shape=VMEM((reps, named, width, BS), BF16),
        in_specs=[whole(SMEM), whole(SMEM), whole()],
        out_specs=whole(),
        compiler_params=pltpu.CompilerParams(vmem_limit_bytes=16 << 20),
        name="select",
    )(names, place, near(table))
    chosen = lax.all_to_all(chosen, "rep", 0, 0, tiled=True)

    gram = summed(gram, "blk_1", (1,))
    gram = summed(gram, "blk_0", (2,))
    gram = summed(gram, "blk_0", (1,))

    head = tensor_blocks[0, : STEP * CHUNK]
    parts = pl.pallas_call(
        contract_kernel,
        out_shape=VMEM((reps, named * width + SUBLANES, BS), F32),
        in_specs=[whole(SMEM), whole(SMEM), whole(), whole(pltpu.HBM), whole()],
        out_specs=whole(),
        scratch_shapes=[
            VMEM((slots, BS, BS, BS), BF16),
            pltpu.SemaphoreType.DMA((slots * BS // (PIECE * CHUNK),)),
            VMEM((slots, 2, BS, rank), F32),
            VMEM((slots, BS, rank), BF16),
            VMEM((slots, BS, rank), BF16),
            VMEM((slots, BS, rank), F32),
            VMEM((slots, BS, rank), F32),
            VMEM((slots, BS, rank), F32),
        ],
        compiler_params=pltpu.CompilerParams(vmem_limit_bytes=32 << 20),
        name="contract",
    )(
        triples,
        slot_count,
        near(head),
        pltpu.with_memory_space_constraint(tensor_blocks, pltpu.HBM),
        near(chosen),
    )
    parts = lax.all_to_all(parts.astype(F16), "rep", 0, 0, tiled=True)

    gram = summed(gram, "blk_0", (4,))
    gram = summed(gram, "blk_1", (2,))
    fitted = pl.pallas_call(
        fit_kernel,
        out_shape=jax.ShapeDtypeStruct((per_owner, width, BS), F32),
        in_specs=[whole(), whole()],
        out_specs=whole(),
        compiler_params=pltpu.CompilerParams(vmem_limit_bytes=16 << 20),
        name="fit",
    )(gram, own_rows)

    held = per_owner * width
    scaled = pl.pallas_call(
        scatter_kernel,
        out_shape=VMEM((owners, held + SUBLANES, BS), F32),
        in_specs=[whole(SMEM), whole(SMEM), whole()],
        out_specs=whole(),
        scratch_shapes=[VMEM((owners * per_owner, width, BS), F32)],
        compiler_params=pltpu.CompilerParams(vmem_limit_bytes=16 << 20),
        name="scatter",
    )(names, place, near(parts.astype(F32)))
    arrived = lax.all_to_all(scaled.astype(F16), BLK, 0, 0, tiled=True)
    arrived = arrived.astype(F32)
    moment = (arrived[:, :held] * jnp.exp2(-arrived[:, held:, :1][:, :1])).sum(0)
    gradient = fitted - moment.reshape(per_owner, width, BS)
    return gradient.swapaxes(0, 1).reshape(width, rows).T


def solution(mesh):
    split = Mesh(mesh.devices.reshape(8, 4, mesh.shape["rep"]), ("blk_0", "blk_1", "rep"))
    in_specs = (P(BLK_REP, None, None, None), P(BLK_REP, None), P(BLK_REP), P(BLK, "rep"))
    out_specs = P(BLK, "rep")
    return jax.shard_map(
        shards, mesh=split, in_specs=in_specs, out_specs=out_specs, check_vma=False
    )
```
